256 devices in a mesh: leaf: 256 (over y, x, z, core).
Axes of the slice: x: 4, y: 4, z: 8, core: 2. Of those that a mesh axis runs over, the one named last changes fastest.
Arguments:
- points: bfloat16 [262144, 512], P('leaf'), may hold values from -6 to 6
- weights: float32 [262144, 64], P('leaf'), may hold values from -6 to 6
- leaf_basis: float32 [262144, 256], P('leaf'), may hold values from -0.1875 to 0.1875
- transfer: float32 [256, 7, 256, 256], P('leaf'), may hold values from -0.375 to 0.375
- skeleton_index: int32 [8, 256, 256], replicated, may hold values from 0 to 1023, as said below
- node_owner: int32 [6, 256], replicated, may hold values from 0 to 63, as said below
- near_list: int32 [256, 3], replicated, may hold values from 0 to 7, as said below
Outputs:
- product: float32 [262144, 64], P('leaf')
The draws below stay inside these ranges and needn't reach their ends.
Inputs may be any that keep to these rules, and one draw needn't show every extreme that they name: `near_list`: entry m > 0 of row i names leaf i XOR m of the same aligned group of 8 leaves; 0 marks an empty slot. The nonzero entries of a row are distinct and number 1 to 3; some row has 3. `skeleton_index`: row 0, column i: 256 distinct row numbers below 1024 within leaf i. Row m >= 1, column s below 256 >> m: 256 distinct row numbers below 512; other columns are unused. `node_owner`: row m - 1, column s below 256 >> m: a number below 2 to the power m; other columns are unused.
All inputs are finite; a program needn't handle non-finite values.
Results may differ from the reference program's by a relative error of at most 0.0018.
Values may be sent and summed in bfloat16 or wider, within the bound.
No kernel may reach another device: no remote copies, remote signals or barrier semaphores. Data moves between devices by JAX's collectives and lax.ppermute only.
A program may use at most 128 MiB of HBM per device.

```python
import jax
import jax.numpy as jnp
from jax import lax

LEAF_PTS = 1024
EMBED = 512
RANK = 256
RHS = 64
GROUP = 8
NEAR_MAX = 3
LEVELS = 8
TOTAL_PTS = 262144
N_LEAF = 256


def draw_skeleton_index(key, part):
    subkeys = jax.random.split(key, LEVELS * N_LEAF)
    leaf_rows = jax.vmap(lambda subkey: jax.random.permutation(subkey, LEAF_PTS)[:RANK])(subkeys[:N_LEAF])
    node_rows = jax.vmap(lambda subkey: jax.random.permutation(subkey, 2 * RANK)[:RANK])(subkeys[N_LEAF:])
    return jnp.concatenate([leaf_rows[None], node_rows.reshape(LEVELS - 1, N_LEAF, RANK)], 0).astype(jnp.int32)


def draw_node_owner(key, part):
    heights = jnp.arange(1, LEVELS - 1, dtype=jnp.int32)
    limits = jnp.left_shift(jnp.ones_like(heights), heights)[:, None]
    raw_values = jax.random.randint(key, (LEVELS - 2, N_LEAF), 0, 1 << 30)
    return (raw_values % limits).astype(jnp.int32)


def draw_near_list(key, part):
    order_key, count_key, heavy_key = jax.random.split(key, 3)
    orders = jax.vmap(lambda subkey: jax.random.permutation(subkey, GROUP - 1) + 1)(jax.random.split(order_key, N_LEAF))
    raw_counts = jax.random.randint(count_key, (N_LEAF,), 0, 20)
    counts = 1 + (raw_counts >= 12).astype(jnp.int32) + (raw_counts >= 17).astype(jnp.int32)
    heavy_leaf = jax.random.randint(heavy_key, (), 0, N_LEAF)
    counts = counts.at[heavy_leaf].set(NEAR_MAX)
    near_slots = jnp.arange(NEAR_MAX, dtype=jnp.int32)
    return jnp.where(near_slots[None, :] < counts[:, None], orders[:, :NEAR_MAX], 0).astype(jnp.int32)


def block_scale(stream_key, dims, shards, least, top_value):
    gain = 1.0
    for dim, parts in shards:
        steps = jax.random.uniform(jax.random.fold_in(jax.random.fold_in(stream_key, 6), dim), (parts,), jnp.float32, least / len(shards), top_value / len(shards))
        gain = gain * jnp.repeat(jnp.exp(steps), dims[dim] // parts).reshape((-1,) + (1,) * (len(dims) - 1 - dim))
    return gain


def scatter_about(own_key, extent, width, bound, cuts=(), kind=jnp.bfloat16):
    level = block_scale(own_key, extent, cuts, -0.22, 0.18) if cuts else 1.0
    entries = jax.random.normal(own_key, extent, jnp.float32) * width * level
    return jnp.minimum(jnp.maximum(entries, -bound), bound).astype(kind)


def setup_inputs(seed: int = 0) -> dict:
    seeds = jax.random.split(jax.random.key(seed), 8)
    return {
        "points": scatter_about(seeds[0], (TOTAL_PTS, EMBED), 1.0, 6.0, ((0, 256),)),
        "weights": scatter_about(seeds[1], (TOTAL_PTS, RHS), 1.0, 6.0, ((0, 256),), jnp.float32),
        "leaf_basis": scatter_about(seeds[2], (TOTAL_PTS, RANK), LEAF_PTS ** -0.5, 0.1875, ((0, 256),), jnp.float32),
        "transfer": scatter_about(seeds[3], (N_LEAF, LEVELS - 1, RANK, RANK), RANK ** -0.5, 0.375, ((0, 256),), jnp.float32),
        "skeleton_index": draw_skeleton_index(jax.random.fold_in(seeds[7], 71), 0),
        "node_owner": draw_node_owner(jax.random.fold_in(seeds[7], 71), 0),
        "near_list": draw_near_list(jax.random.fold_in(seeds[7], 71), 0),
    }


PRECISE = lax.Precision.HIGHEST


def kernel_block(left_rows, right_rows):
    scale_factor = 2.0 / left_rows.shape[1]
    left_norm = jnp.sum(jnp.square(left_rows.astype(jnp.float32)), axis=1)
    right_norm = jnp.sum(jnp.square(right_rows.astype(jnp.float32)), axis=1)
    inner_products = lax.dot_general(left_rows, right_rows, (((1,), (1,)), ((), ())), preferred_element_type=jnp.float32)
    return jnp.exp(-scale_factor * (left_norm[:, None] + right_norm[None, :] - 2.0 * inner_products))


def apply_matrix(matrix, values):
    return jnp.dot(matrix, values, precision=PRECISE, preferred_element_type=jnp.float32)


def pick_rows(blocks, picks):
    return jax.vmap(lambda block_rows, row_picks: jnp.take(block_rows, row_picks, axis=0))(blocks, picks)


def owner_of(height, node_count, node_owner):
    node_ids = jnp.arange(node_count, dtype=jnp.int32) * (1 << height)
    if height == 0:
        return node_ids
    return node_ids + node_owner[height - 1, :node_count]


def reference(points, weights, leaf_basis, transfer, skeleton_index, node_owner, near_list):
    leaf_points = points.reshape(N_LEAF, LEAF_PTS, EMBED)
    leaf_weights = weights.reshape(N_LEAF, LEAF_PTS, RHS)
    leaf_bases = leaf_basis.reshape(N_LEAF, LEAF_PTS, RANK)
    leaf_ids = jnp.arange(N_LEAF, dtype=jnp.int32)

    def near_leaf(leaf_number):
        own_points = leaf_points[leaf_number]
        running_sum = apply_matrix(kernel_block(own_points, own_points), leaf_weights[leaf_number])
        for near_slot in range(NEAR_MAX):
            offset = near_list[leaf_number, near_slot]
            partner = jnp.bitwise_xor(leaf_number, offset)
            near_term = apply_matrix(kernel_block(own_points, leaf_points[partner]), leaf_weights[partner])
            running_sum = running_sum + jnp.where(offset > 0, near_term, 0.0)
        return running_sum

    near_part = lax.map(near_leaf, leaf_ids)

    node_coeff = jnp.einsum("nlk,nlr->nkr", leaf_bases, leaf_weights, precision=PRECISE)
    node_rows = pick_rows(leaf_points, skeleton_index[0])
    level_coeff = []
    level_rows = []
    for height in range(LEVELS):
        level_coeff.append(node_coeff)
        level_rows.append(node_rows)
        if height + 1 < LEVELS:
            node_count = N_LEAF >> height
            transfer_stack = transfer[owner_of(height, node_count, node_owner), height]
            lifted = jnp.einsum("nkj,nkr->njr", transfer_stack, node_coeff, precision=PRECISE)
            node_coeff = lifted[0::2] + lifted[1::2]
            joined = jnp.concatenate([node_rows[0::2], node_rows[1::2]], axis=1)
            node_rows = pick_rows(joined, skeleton_index[height + 1, : node_count // 2])

    def sibling_coupling(height):
        rows_here = level_rows[height]
        coeff_here = level_coeff[height]
        sibling = jnp.bitwise_xor(jnp.arange(rows_here.shape[0], dtype=jnp.int32), 1)
        blocks = jax.vmap(kernel_block)(rows_here, rows_here[sibling])
        return jnp.einsum("nkj,njr->nkr", blocks, coeff_here[sibling], precision=PRECISE)

    down_field = sibling_coupling(LEVELS - 1)
    for height in range(LEVELS - 2, -1, -1):
        node_count = N_LEAF >> height
        transfer_stack = transfer[owner_of(height, node_count, node_owner), height]
        down_field = jnp.einsum("nkj,njr->nkr", transfer_stack, jnp.repeat(down_field, 2, axis=0), precision=PRECISE)
        if height >= 3:
            down_field = down_field + sibling_coupling(height)

    def far_leaf(leaf_number):
        own_rows = level_rows[0][leaf_number]
        group_start = leaf_number - leaf_number % GROUP
        running_sum = jnp.zeros((RANK, RHS), jnp.float32)
        for target in range(GROUP):
            partner = group_start + target
            offset = jnp.bitwise_xor(leaf_number, partner)
            distant = (offset != 0) & jnp.logical_not(jnp.any(near_list[leaf_number] == offset))
            far_term = apply_matrix(kernel_block(own_rows, level_rows[0][partner]), level_coeff[0][partner])
            running_sum = running_sum + jnp.where(distant, far_term, 0.0)
        return running_sum

    down_field = down_field + lax.map(far_leaf, leaf_ids)
    far_part = jnp.einsum("nlk,nkr->nlr", leaf_bases, down_field, precision=PRECISE)
    return (near_part + far_part).reshape(N_LEAF * LEAF_PTS, RHS)
```

```python
import jax
import jax.numpy as jnp
from jax import lax
from jax.experimental import pallas as pl
from jax.experimental.pallas import tpu as pltpu
from jax.sharding import PartitionSpec as P

GROUP = 8
PTS = 1024
DIM = 512
RANK = 256
RHS = 64
ROWS = PTS + 4 * RHS + RHS
SCALE = 2.0 / DIM
INTERPRET = False

F32 = jnp.float32
BF16 = jnp.bfloat16
NN = (((1,), (0,)), ((), ()))
NT = (((1,), (1,)), ((), ()))


def mm(a, b, dims=NN):
    return lax.dot_general(a, b, dims, preferred_element_type=F32)


def split(a):
    high = a.astype(BF16)
    return high, (a - high.astype(F32)).astype(BF16)


def product(a, b, dims=NN):
    a_high, a_low = split(a)
    b_high, b_low = split(b)
    rows = a.shape[0]
    both = mm(jnp.concatenate([a_high, a_low], 0), b_high, dims)
    return both[:rows] + both[rows:] + mm(a_high, b_low, dims)


def row_norms(rows):
    wide = rows.astype(F32)
    high, low = split(wide * wide)
    ones = jnp.ones((8, rows.shape[1]), BF16)
    return mm(ones, high, NT) + mm(ones, low, NT)


def kern(left, right, right_norm):
    wide = left.astype(F32)
    left_norm = jnp.sum(wide * wide, axis=1, keepdims=True)
    inner = mm(left, right, NT)
    return jnp.exp(-SCALE * (left_norm + right_norm - 2.0 * inner))


def pick_matrix(picks, count):
    lanes = lax.broadcasted_iota(jnp.int32, (picks.shape[0], count), 1)
    return jnp.where(lanes == picks, 1.0, 0.0).astype(BF16)


def weighted(values, block):
    half = values.shape[0] // 2
    high, low = split(block)
    both = mm(values, high)
    return both[:half] + both[half:] + mm(values[:half], low)


def call(body, outs, args, smem=0, flops=0, grant=None):
    in_specs = [
        pl.BlockSpec(memory_space=pltpu.SMEM) if k < smem else pl.BlockSpec(memory_space=pltpu.VMEM)
        for k in range(len(args))
    ]
    size = sum(a.size * a.dtype.itemsize for a in args)
    return pl.pallas_call(
        body,
        out_shape=[jax.ShapeDtypeStruct(s, d) for s, d in outs],
        in_specs=in_specs,
        out_specs=[pl.BlockSpec(memory_space=pltpu.VMEM) for _ in outs],
        compiler_params=pltpu.CompilerParams(vmem_limit_bytes=grant or (40 << 20)),
        cost_estimate=pl.CostEstimate(flops=flops, transcendentals=0, bytes_accessed=size),
        interpret=INTERPRET,
    )(*args)


def prepare_body(x_ref, b_ref, v_ref, col_ref, p_ref, w_ref, z_ref, nx_ref, nz_ref):
    x = x_ref[...]
    z = mm(pick_matrix(col_ref[:, 0:1], PTS), x).astype(BF16)
    z_ref[...] = z
    b_high, b_low = split(b_ref[...])
    v_high, v_low = split(v_ref[...])
    both = mm(jnp.concatenate([b_high, b_low], 0), v_high)
    w = both[:RHS] + both[RHS:] + mm(b_high, v_low)
    w_ref[...] = w
    w_high, w_low = split(w)
    p_ref[0:PTS, :] = x
    for k, part in enumerate((b_high[:, :DIM], b_low[:, :DIM], b_high[:, DIM:], b_low[:, DIM:])):
        p_ref[PTS + k * RHS : PTS + (k + 1) * RHS, :] = part
    p_ref[PTS + 4 * RHS :, 0:RANK] = w_high
    p_ref[PTS + 4 * RHS :, RANK:] = w_low
    nx_ref[...] = row_norms(x)
    nz_ref[...] = row_norms(z)


def add_near(p_ref, x_ref, nx_ref, near_ref):
    total = near_ref[...]
    x = x_ref[...]
    norm = nx_ref[0:1, :]
    for k in range(4):
        block = kern(p_ref[k * 256 : (k + 1) * 256, :], x, norm)
        top = PTS + (k // 2) * 2 * RHS
        values = p_ref[top : top + 2 * RHS, (k % 2) * 256 : (k % 2 + 1) * 256]
        total = total + weighted(values, block)
    near_ref[...] = total


def add_far(p_ref, picks, z_ref, nz_ref, far_ref):
    z = mm(pick_matrix(picks, PTS), p_ref[0:PTS, :]).astype(BF16)
    block = kern(z, z_ref[...], nz_ref[0:1, :])
    w = p_ref[PTS + 4 * RHS :, :]
    values = jnp.concatenate([w[:, :RANK], w[:, RANK:]], 0)
    far_ref[...] += weighted(values, block)


def group_body(slots, own, flag_ref, x_ref, nx_ref, z_ref, nz_ref, col_ref, near_in, far_in, *refs):
    near_ref, far_ref = refs[-2:]
    near_ref[...] = near_in[...]
    far_ref[...] = far_in[...]
    if own:
        add_near(refs[0], x_ref, nx_ref, near_ref)
    for k, slot in enumerate(slots):
        p_ref = refs[k + own]

        @pl.when(flag_ref[slot] == 1)
        def _():
            add_near(p_ref, x_ref, nx_ref, near_ref)

        @pl.when(flag_ref[slot] == 2)
        def _():
            add_far(p_ref, col_ref[:, 8 + slot : 9 + slot], z_ref, nz_ref, far_ref)


def node_body(height, last, flag_ref, col_ref, own_ref, sib_ref, *outs):
    own = own_ref[...]
    sib = sib_ref[...]
    outs = list(outs)
    if not last:
        upper = flag_ref[16 + height] * RANK
        picks = col_ref[:, height + 1 : height + 2]
        rows = mm(pick_matrix(picks - upper, RANK), own) + mm(pick_matrix(picks - (RANK - upper), RANK), sib)
        outs.pop(0)[...] = rows.astype(BF16)
    if height >= 3:
        outs.pop(0)[...] = kern(sib, own, row_norms(own)[0:1, :])


def final_body(levels, near_ref, far_ref, v_ref, t_ref, e_ref, *refs):
    out_ref = refs[-1]
    blocks = refs[0 : levels - 3]
    coeffs = refs[levels - 3 : -1]
    field = product(coeffs[-1][...], blocks[-1][...])
    for height in range(levels - 2, -1, -1):
        matrix = e_ref[height - 1] if height else t_ref[0]
        field = product(field, matrix, NT)
        if height >= 3:
            field = field + product(coeffs[height - 3][...], blocks[height - 3][...])
    field = field + far_ref[...]
    out_ref[...] = near_ref[...] + product(field, v_ref[...], NT)


def per_device(points, weights, leaf_basis, transfer, skeleton_index, node_owner, near_list):
    count = lax.axis_size("leaf")
    levels = count.bit_length() - 1
    leaf = lax.axis_index("leaf")
    bits = [leaf >> b & 1 for b in range(levels)]
    core = bits[0]
    line = leaf >> 1 & 3
    start = leaf - leaf % GROUP

    def swap(value, bit):
        return lax.ppermute(value, "leaf", [(s, s ^ (1 << bit)) for s in range(count)])

    def shift(value, step, lines):
        return lax.ppermute(value, "leaf", [(s, s + 2 * step) for s in range(count) if (s >> 1 & 3) in lines])

    places = jnp.stack([line, line - 1, line - 1, line + 1, line + 1]
                       + [jnp.where(line >= 2, line - 2, line + 2)] * 2
                       + [jnp.where(line == 3, 0, jnp.where(line == 0, 3, -1))] * 2)
    cores = core ^ jnp.array([1, 0, 1, 0, 1, 0, 1, 0, 1], jnp.int32)
    there = (places >= 0) & (places <= 3)
    targets = jnp.where(there, places, 0) * 2 + cores
    offsets = targets ^ (leaf % GROUP)
    near_row = near_list[leaf]
    listed = jnp.any(near_row[None, :] == offsets[:, None], axis=1)
    kinds = jnp.where(there, jnp.where(listed, 1, 2), 0).astype(jnp.int32)
    flags = jnp.concatenate([kinds, jnp.zeros((7,), jnp.int32), jnp.stack(bits).astype(jnp.int32)])
    heights = jnp.arange(levels)
    path = heights * skeleton_index.shape[1] + (leaf >> heights)
    path = jnp.concatenate([path, jnp.zeros((8 - levels,), path.dtype), start + targets])
    cols = jnp.take(skeleton_index.reshape(-1, RANK), path, axis=0).T

    weights_t = weights.T
    payload, w, z, norm_x, norm_z = call(
        prepare_body,
        [((ROWS, DIM), BF16), ((RHS, RANK), F32), ((RANK, DIM), BF16), ((8, PTS), F32), ((8, RANK), F32)],
        [points, weights_t, leaf_basis, cols],
        flops=2 * 10**9,
    )

    def group(slots, own, near, far, payloads):
        return call(
            lambda *refs: group_body(slots, own, *refs),
            [((RHS, PTS), F32), ((RHS, RANK), F32)],
            [flags, points, norm_x, z, norm_z, cols, near, far] + payloads,
            smem=1,
            flops=3 * 10**9 * len(payloads),
        )

    partner = swap(payload, 0)
    right1 = shift(payload, 1, (0, 1, 2))
    left1 = shift(payload, -1, (1, 2, 3))
    right2 = shift(right1, 1, (1, 2))
    left2 = shift(left1, -1, (1, 2))
    two = jnp.where(line >= 2, right2, left2)
    three = lax.ppermute(
        two, "leaf",
        [(s, s + 2) if (s >> 1 & 3) == 2 else (s, s - 2) for s in range(count) if (s >> 1 & 3) in (1, 2)],
    )
    near = jnp.zeros((RHS, PTS), F32)
    far = jnp.zeros((RHS, RANK), F32)
    near, far = group((0,), 1, near, far, [payload, partner])
    near, far = group((1, 2, 3, 4), 0, near, far, [right1, swap(right1, 0), left1, swap(left1, 0)])
    near, far = group((5, 6), 0, near, far, [two, swap(two, 0)])
    near, far = group((7, 8), 0, near, far, [three, swap(three, 0)])

    def half(array, bit, other):
        size = array.shape[1] // 2
        place = (1 - bits[bit]) if other else bits[bit]
        return lax.dynamic_slice_in_dim(array, place * size, size, 1)

    def whole(array, bit):
        arrived = swap(array, bit)
        upper = bits[bit] == 1
        return jnp.concatenate([jnp.where(upper, arrived, array), jnp.where(upper, array, arrived)], 1)

    owned = jnp.stack([leaf % (1 << h) == node_owner[h - 1, leaf >> h] for h in range(1, levels - 1)])
    masked = jnp.where(owned[:, None, None], transfer[0, 1 : levels - 1], 0.0)
    part0 = half(masked, 0, False) + swap(half(masked, 0, True), 0)
    rest = part0[1:]
    part1 = half(rest, 1, False) + swap(half(rest, 1, True), 1)
    rest = part1[1:]
    part2 = half(rest, 2, False) + swap(half(rest, 2, True), 2)
    done = []
    for bit in range(3, levels - 2):
        done.append(part2[:1])
        part2 = part2[1:]
        part2 = part2 + swap(part2, bit)
    part2 = jnp.concatenate(done + [part2], 0)
    part1 = jnp.concatenate([part1[:1], whole(part2, 2)], 0)
    part0 = jnp.concatenate([part0[:1], whole(part1, 1)], 0)
    spread = whole(part0, 0)

    blocks = []
    rows = z
    for height in range(levels):
        last = height + 1 == levels
        outs = ([] if last else [((RANK, DIM), BF16)]) + ([((RANK, RANK), F32)] if height >= 3 else [])
        result = call(
            lambda *refs: node_body(height, last, *refs),
            outs,
            [flags, cols, rows, swap(rows, height)],
            smem=1,
            flops=5 * 10**8,
        )
        if height >= 3:
            blocks.append(result[-1])
        rows = result[0]

    coeffs = []
    for height in range(levels):
        if height >= 3:
            coeffs.append(swap(w, height))
        if height + 1 < levels:
            matrix = spread[height - 1] if height else transfer[0, 0]
            lifted = jnp.dot(w, matrix, precision=lax.Precision.HIGHEST, preferred_element_type=F32)
            w = lifted + swap(lifted, height)

    out = call(
        lambda *refs: final_body(levels, *refs),
        [((RHS, PTS), F32)],
        [near, far, leaf_basis, transfer[0, 0:1], spread] + blocks + coeffs,
        flops=10**9,
    )[0]
    return out.T


def solution(mesh):
    return jax.shard_map(
        per_device,
        mesh=mesh,
        in_specs=(
            P("leaf", None),
            P("leaf", None),
            P("leaf", None),
            P("leaf", None, None, None),
            P(),
            P(),
            P(),
        ),
        out_specs=P("leaf", None),
        check_vma=False,
    )
```

```python
import jax
import jax.numpy as jnp
from jax import lax
from jax.experimental import pallas as pl
from jax.experimental.pallas import tpu as pltpu
from jax.sharding import PartitionSpec as P

GROUP = 8
PTS = 1024
DIM = 512
RANK = 256
RHS = 64
ROWS = PTS + 4 * RHS + RHS
SCALE = 2.0 / DIM
INTERPRET = False

SIDE = 7
PROXY = 8
BITS = 16
CORE = BITS
OWNED = 24

F32 = jnp.float32
BF16 = jnp.bfloat16
NN = (((1,), (0,)), ((), ()))
NT = (((1,), (1,)), ((), ()))


def mm(a, b, dims=NN):
    return lax.dot_general(a, b, dims, preferred_element_type=F32)


def split(a):
    high = a.astype(BF16)
    return high, (a - high.astype(F32)).astype(BF16)


def product(a, b, dims=NN):
    a_high, a_low = split(a)
    b_high, b_low = split(b)
    rows = a.shape[0]
    both = mm(jnp.concatenate([a_high, a_low], 0), b_high, dims)
    return both[:rows] + both[rows:] + mm(a_high, b_low, dims)


def row_norms(rows):
    wide = rows.astype(F32)
    high, low = split(wide * wide)
    ones = jnp.ones((8, rows.shape[1]), BF16)
    return mm(ones, high, NT) + mm(ones, low, NT)


def kern(left, right, right_norm):
    wide = left.astype(F32)
    left_norm = jnp.sum(wide * wide, axis=1, keepdims=True)
    inner = mm(left, right, NT)
    return jnp.exp(-SCALE * (left_norm + right_norm - 2.0 * inner))


def pick_matrix(picks, count):
    lanes = lax.broadcasted_iota(jnp.int32, (picks.shape[0], count), 1)
    return jnp.where(lanes == picks, 1.0, 0.0).astype(BF16)


def weighted(values, block):
    half = values.shape[0] // 2
    high, low = split(block)
    both = mm(values, high)
    return both[:half] + both[half:] + mm(values[:half], low)


def call(body, outs, args, smem=0, flops=0, far=0, scratch=()):
    near = len(args) - far
    in_specs = [
        pl.BlockSpec(memory_space=pltpu.SMEM if k < smem else pltpu.VMEM if k < near else pltpu.HBM)
        for k in range(len(args))
    ]
    size = sum(a.size * a.dtype.itemsize for a in args)
    return pl.pallas_call(
        body,
        out_shape=[jax.ShapeDtypeStruct(s, d) for s, d in outs],
        in_specs=in_specs,
        out_specs=[pl.BlockSpec(memory_space=pltpu.VMEM) for _ in outs],
        scratch_shapes=list(scratch),
        compiler_params=pltpu.CompilerParams(vmem_limit_bytes=40 << 20),
        cost_estimate=pl.CostEstimate(flops=flops, transcendentals=0, bytes_accessed=size),
        interpret=INTERPRET,
    )(*args)


def lift(values, pair):
    high, low = split(values)
    rows = values.shape[0]
    both = mm(jnp.concatenate([high, low], 0), pair[:, :RANK])
    return both[:rows] + both[rows:] + mm(high, pair[:, RANK:])


def lower(values, pair):
    high, low = split(values)
    rows = values.shape[0]
    both = mm(jnp.concatenate([high, low], 0), pair[:, :RANK], NT)
    return both[:rows] + both[rows:] + mm(high, pair[:, RANK:], NT)


def prepare_body(x_ref, b_ref, v_ref, p_ref, w_ref, nx_ref):
    x = x_ref[...]
    b_high, b_low = split(b_ref[...])
    v_high, v_low = split(v_ref[...])
    both = mm(jnp.concatenate([b_high, b_low], 0), v_high)
    w = both[:RHS] + both[RHS:] + mm(b_high, v_low)
    w_ref[...] = w
    w_high, w_low = split(w)
    p_ref[0:PTS, :] = x
    for k, part in enumerate((b_high[:, :DIM], b_low[:, :DIM], b_high[:, DIM:], b_low[:, DIM:])):
        p_ref[PTS + k * RHS : PTS + (k + 1) * RHS, :] = part
    p_ref[PTS + 4 * RHS :, 0:RANK] = w_high
    p_ref[PTS + 4 * RHS :, RANK:] = w_low
    nx_ref[...] = row_norms(x)


def skeleton_body(x_ref, col_ref, w_ref, t_ref, z_ref, nz_ref, lifted_ref):
    z = mm(pick_matrix(col_ref[:, 0:1], PTS), x_ref[...]).astype(BF16)
    z_ref[...] = z
    nz_ref[...] = row_norms(z)
    lifted_ref[...] = product(w_ref[...], t_ref[0])


def add_near(p_ref, x, norm, near_ref):
    total = near_ref[...]
    for k in range(4):
        block = kern(p_ref[k * 256 : (k + 1) * 256, :], x, norm)
        top = PTS + (k // 2) * 2 * RHS
        values = p_ref[top : top + 2 * RHS, (k % 2) * 256 : (k % 2 + 1) * 256]
        total = total + weighted(values, block)
    near_ref[...] = total


def add_far(p_ref, picks, z, norm, far_ref):
    rows = mm(pick_matrix(picks, PTS), p_ref[0:PTS, :]).astype(BF16)
    block = kern(rows, z, norm)
    w = p_ref[PTS + 4 * RHS :, :]
    values = jnp.concatenate([w[:, :RANK], w[:, RANK:]], 0)
    far_ref[...] += weighted(values, block)


def self_body(flag_ref, x_ref, nx_ref, z_ref, nz_ref, col_ref, own_ref, other_ref, near_ref, far_ref):
    near_ref[...] = jnp.zeros_like(near_ref)
    far_ref[...] = jnp.zeros_like(far_ref)
    add_near(own_ref, x_ref[...], nx_ref[0:1, :], near_ref)

    @pl.when(flag_ref[0] == 1)
    def _():
        add_near(other_ref, x_ref[...], nx_ref[0:1, :], near_ref)

    @pl.when(flag_ref[0] == 2)
    def _():
        add_far(other_ref, col_ref[:, 8:9], z_ref[...], nz_ref[0:1, :], far_ref)


def fetch(flag_ref, first, second, buffer, semaphore):
    @pl.when(flag_ref[CORE] == 0)
    def _():
        copy = pltpu.make_async_copy(first, buffer, semaphore)
        copy.start()
        copy.wait()

    @pl.when(flag_ref[CORE] == 1)
    def _():
        copy = pltpu.make_async_copy(second, buffer, semaphore)
        copy.start()
        copy.wait()


def group_body(slots, flag_ref, x_ref, nx_ref, z_ref, nz_ref, col_ref, near_in, far_in, *refs):
    near_ref, far_ref, buffer, semaphore = refs[-4:]
    near_ref[...] = near_in[...]
    far_ref[...] = far_in[...]
    for k, slot in enumerate(slots):

        @pl.when(flag_ref[slot] > 0)
        def _():
            fetch(flag_ref, refs[2 * k], refs[2 * k + 1], buffer, semaphore)

        @pl.when(flag_ref[slot] == 1)
        def _():
            add_near(buffer, x_ref[...], nx_ref[0:1, :], near_ref)

        @pl.when(flag_ref[slot] == 2)
        def _():
            add_far(buffer, col_ref[:, 8 + slot : 9 + slot], z_ref[...], nz_ref[0:1, :], far_ref)


def proxy_body(flag_ref, col_ref, *refs):
    out_ref, ends, buffer, near_ref, far_ref, z_ref, semaphore = refs[-7:]
    core = flag_ref[CORE]
    near_ref[...] = jnp.zeros_like(near_ref)
    far_ref[...] = jnp.zeros_like(far_ref)

    def load(source, target):
        copy = pltpu.make_async_copy(source, target, semaphore)
        copy.start()
        copy.wait()

    for k, side in enumerate((1, 2)):

        @pl.when((flag_ref[SIDE] == side) & (core == 0))
        def _():
            load(refs[4 * k], ends)

        @pl.when((flag_ref[SIDE] == side) & (core == 1))
        def _():
            load(refs[4 * k + 3], ends)

    @pl.when(flag_ref[SIDE] > 0)
    def _():
        x = ends[0:PTS, :]
        norm = row_norms(x)[0:1, :]
        z_ref[...] = mm(pick_matrix(col_ref[:, 15:16], PTS), x).astype(BF16)
        z_norm = row_norms(z_ref[...])[0:1, :]
        for k in range(2):
            fetch(flag_ref, refs[8 + 2 * k], refs[9 + 2 * k], buffer, semaphore)

            @pl.when(flag_ref[PROXY + k] == 1)
            def _():
                add_near(buffer, ends[0:PTS, :], norm, near_ref)

            @pl.when(flag_ref[PROXY + k] == 2)
            def _():
                add_far(buffer, col_ref[:, 13 + k : 14 + k], z_ref[...], z_norm, far_ref)

    out_ref[:, 0:PTS] = near_ref[...]
    out_ref[:, PTS:] = far_ref[...]


def node_body(height, last, flag_ref, col_ref, own_ref, sib_ref, *outs):
    outs = list(outs)

    @pl.when((flag_ref[CORE] == 1) | (height == 0))
    def _():
        rest = list(outs)
        own = own_ref[...]
        sib = sib_ref[...]
        if not last:
            upper = flag_ref[BITS + height] * RANK
            picks = col_ref[:, height + 1 : height + 2]
            rows = mm(pick_matrix(picks - upper, RANK), own) + mm(pick_matrix(picks - (RANK - upper), RANK), sib)
            rest.pop(0)[...] = rows.astype(BF16)
        if height >= 3:
            rest.pop(0)[...] = kern(sib, own, row_norms(own)[0:1, :])


def mask_body(flag_ref, t_ref, out_ref):
    for k in range(out_ref.shape[0]):
        high, low = split(jnp.where(flag_ref[OWNED + k] == 1, t_ref[k + 1], 0.0))
        out_ref[k, :, 0:RANK] = high
        out_ref[k, :, RANK:] = low


def halve_body(bit, flag_ref, held_ref, arrived_ref, done_ref, keep_ref, send_ref):
    size = keep_ref.shape[1]
    upper = flag_ref[BITS + bit]
    done_ref[...] = held_ref[0] + arrived_ref[0]
    keep = pl.ds(pl.multiple_of(upper * size, 16), size)
    send = pl.ds(pl.multiple_of((1 - upper) * size, 16), size)
    keep_ref[...] = held_ref[1:, keep, :] + arrived_ref[1:, keep, :]
    send_ref[...] = held_ref[1:, send, :] + arrived_ref[1:, send, :]


def add_body(held_ref, arrived_ref, done_ref, *rest):
    total = held_ref[...] + arrived_ref[...]
    done_ref[...] = total[0]
    if rest:
        rest[0][...] = total[1:]


def join_body(bit, parts, flag_ref, *refs):
    out_ref = refs[-1]
    arrived_ref = refs[parts]
    lead = len(refs) - parts - 2
    if lead:
        out_ref[0] = refs[parts + 1][...]
    size = arrived_ref.shape[1]
    upper = flag_ref[BITS + bit]
    mine = pl.ds(pl.multiple_of(upper * size, 16), size)
    theirs = pl.ds(pl.multiple_of((1 - upper) * size, 16), size)
    total = arrived_ref.shape[0]
    for k in range(total):
        held = refs[k][...] if parts > 1 else refs[0][k]
        out_ref[lead + k, mine, :] = held
        out_ref[lead + k, theirs, :] = arrived_ref[k]


def climb_body(lifted_ref, arrived_ref, pair_ref, out_ref):
    w = lifted_ref[...] + arrived_ref[...]
    rows = out_ref.shape[0]
    if rows > RHS:
        out_ref[RHS:, :] = w
    out_ref[0:RHS, :] = lift(w, pair_ref[...])


def descend_body(levels, flag_ref, pairs_ref, first_ref, *refs):
    out_ref = refs[-1]
    blocks = refs[0 : levels - 3]
    coeffs = refs[levels - 3 : -1]

    @pl.when(flag_ref[CORE] == 1)
    def _():
        def coupling(height):
            values = coeffs[height - 3]
            values = values[RHS:, :] if values.shape[0] > RHS else values[...]
            return product(values, blocks[height - 3][...])

        field = coupling(levels - 1)
        for height in range(levels - 2, 0, -1):
            field = lower(field, pairs_ref[height - 2] if height > 1 else first_ref[...])
            if height >= 3:
                field = field + coupling(height)
        out_ref[...] = field


def final_body(flag_ref, near_ref, far_ref, proxy_ref, v_ref, t_ref, held_ref, arrived_ref, out_ref):
    parent = jnp.where(flag_ref[CORE] == 1, held_ref[...], arrived_ref[...])
    field = product(parent, t_ref[0], NT) + far_ref[...] + proxy_ref[:, PTS:]
    out_ref[...] = near_ref[...] + proxy_ref[:, 0:PTS] + product(field, v_ref[...], NT)


def per_device(points, weights, leaf_basis, transfer, skeleton_index, node_owner, near_list):
    count = lax.axis_size("leaf")
    levels = count.bit_length() - 1
    leaf = lax.axis_index("leaf")
    bits = [leaf >> b & 1 for b in range(levels)]
    core = bits[0]
    line = leaf >> 1 & 3
    start = leaf - leaf % GROUP
    everyone = range(count)

    def swap(value, bit):
        return lax.ppermute(value, "leaf", [(s, s ^ (1 << bit)) for s in everyone])

    def cross(value, bit):
        return lax.ppermute(value, "leaf", [(s, s ^ (1 << bit)) for s in everyone if s & 1])

    def shift(value, step, lines):
        return lax.ppermute(
            value, "leaf", [(s, s + 2 * step) for s in everyone if s & 1 == 0 and (s >> 1 & 3) in lines]
        )

    def hand_over(value):
        return lax.ppermute(value, "leaf", [(s, s + 1) for s in everyone if s & 1 == 0])

    payload, w, norm_x = call(
        prepare_body,
        [((ROWS, DIM), BF16), ((RHS, RANK), F32), ((8, PTS), F32)],
        [points, weights.T, leaf_basis],
        flops=10**9,
    )
    partner = swap(payload, 0)
    right1 = [shift(payload, 1, (0, 1, 2)), shift(partner, 1, (0, 1, 2))]
    left1 = [shift(payload, -1, (1, 2, 3)), shift(partner, -1, (1, 2, 3))]
    right2 = [shift(v, 1, (1, 2)) for v in right1]
    left2 = [shift(v, -1, (1, 2)) for v in left1]
    two = [jnp.where(line >= 2, r, l) for r, l in zip(right2, left2)]

    far_end = jnp.where(line >= 2, line - 2, line + 2)
    places = jnp.stack([line, line - 1, line - 1, line + 1, line + 1, far_end, far_end])
    cores = jnp.stack([1 - core] + [jnp.int32(0), jnp.int32(1)] * 3)
    there = (places >= 0) & (places <= 3)
    targets = jnp.where(there, places, 0) * 2 + cores
    client_line = jnp.where(line == 2, 3, 0)
    client = start + client_line * 2 + core
    works = (line == 1) | (line == 2)

    def kinds_of(row_leaf, spots, valid):
        row = lax.dynamic_slice(near_list, (row_leaf, 0), (1, 3))
        listed = jnp.any(row == (spots ^ (row_leaf % GROUP))[:, None], axis=1)
        return jnp.where(valid, jnp.where(listed, 1, 2), 0).astype(jnp.int32)

    kinds = kinds_of(leaf, targets, there)
    ends = kinds_of(client, targets[5:7], works)
    side = jnp.where(line == 1, 1, jnp.where(line == 2, 2, 0))
    owned = jnp.stack([(leaf % (1 << h) == node_owner[h - 1, leaf >> h]).astype(jnp.int32) for h in range(1, levels - 1)])
    flags = jnp.concatenate(
        [kinds, side[None], ends, jnp.zeros((BITS - PROXY - 2,), jnp.int32), jnp.stack(bits),
         jnp.zeros((OWNED - BITS - levels,), jnp.int32), owned]
    ).astype(jnp.int32)
    heights = jnp.arange(levels)
    path = heights * skeleton_index.shape[1] + (leaf >> heights)
    path = jnp.concatenate([path, jnp.zeros((8 - levels,), path.dtype), start + targets, client[None]])
    cols = jnp.take(skeleton_index.reshape(-1, RANK), path, axis=0).T

    matrices = transfer[0]
    upper = levels - 2
    masked = call(mask_body, [((upper, RANK, 2 * RANK), BF16)], [flags, matrices], smem=1)[0]
    pair = lambda n, rows: ((n, rows, 2 * RANK), BF16)
    one = lambda rows: ((rows, 2 * RANK), BF16)
    first, keep, send = call(
        lambda *r: halve_body(1, *r),
        [one(256), pair(upper - 1, 128), pair(upper - 1, 128)],
        [flags, masked, hand_over(masked)], smem=1,
    )
    second, keep, send = call(
        lambda *r: halve_body(2, *r),
        [one(128), pair(upper - 2, 64), pair(upper - 2, 64)],
        [flags, keep, cross(send, 1)], smem=1,
    )
    arrived = cross(send, 2)
    thirds = []
    for bit in range(3, levels - 1):
        rest = keep.shape[0] - 1
        result = call(add_body, [one(64)] + ([pair(rest, 64)] if rest else []), [keep, arrived])
        thirds.append(result[0])
        if rest:
            keep = result[1]
            arrived = cross(keep, bit)
    stacked = jnp.stack(thirds)
    joined = call(
        lambda *r: join_body(2, 1, *r), [pair(upper - 1, 128)],
        [flags, stacked, cross(stacked, 2), second], smem=1,
    )[0]
    pairs = call(
        lambda *r: join_body(1, 1, *r), [pair(upper - 1, 256)], [flags, joined, cross(joined, 1)], smem=1,
    )[0]

    z, norm_z, lifted = call(
        skeleton_body,
        [((RANK, DIM), BF16), ((8, RANK), F32), ((RHS, RANK), F32)],
        [points, cols, w, matrices[0:1]],
    )

    blocks = []
    rows = z
    for height in range(levels):
        last = height + 1 == levels
        outs = ([] if last else [((RANK, DIM), BF16)]) + ([((RANK, RANK), F32)] if height >= 3 else [])
        result = call(
            lambda *refs: node_body(height, last, *refs),
            outs,
            [flags, cols, rows, cross(rows, height) if height else swap(rows, 0)],
            smem=1,
            flops=5 * 10**8,
        )
        if height >= 3:
            blocks.append(result[-1])
        rows = result[0]

    coeffs = []
    arrived = swap(lifted, 0)
    for height in range(1, levels - 1):
        matrix = first if height == 1 else pairs[height - 2]
        rows_out = 2 * RHS if height >= 3 else RHS
        lifted = call(climb_body, [((rows_out, RANK), F32)], [lifted[:RHS], arrived[:RHS], matrix])[0]
        arrived = cross(lifted, height)
        if height >= 3:
            coeffs.append(arrived)
    top = lifted[:RHS] + arrived[:RHS]
    coeffs.append(cross(top, levels - 1))
    parent = call(
        lambda *refs: descend_body(levels, *refs),
        [((RHS, RANK), F32)],
        [flags, pairs, first] + blocks + coeffs,
        smem=1,
    )[0]
    parent_other = lax.ppermute(parent, "leaf", [(s, s - 1) for s in everyone if s & 1])

    near, far = call(
        self_body, [((RHS, PTS), F32), ((RHS, RANK), F32)],
        [flags, points, norm_x, z, norm_z, cols, payload, partner], smem=1, flops=5 * 10**9,
    )
    first_arrivals = []
    for value in right1 + left1:
        first_arrivals += [value, hand_over(value)]
    second_arrivals = []
    for value in two:
        second_arrivals += [value, hand_over(value)]
    scratch = [pltpu.VMEM((ROWS, DIM), BF16)]
    proxy = call(
        proxy_body, [((RHS, PTS + RANK), F32)], [flags, cols] + first_arrivals + second_arrivals,
        smem=1, flops=5 * 10**9, far=12,
        scratch=scratch * 2 + [pltpu.VMEM((RHS, PTS), F32), pltpu.VMEM((RHS, RANK), F32),
                               pltpu.VMEM((RANK, DIM), BF16), pltpu.SemaphoreType.DMA],
    )[0]
    proxy = lax.ppermute(
        proxy, "leaf",
        [(s, s + 2) if (s >> 1 & 3) == 2 else (s, s - 2) for s in everyone if (s >> 1 & 3) in (1, 2)],
    )

    def group(slots, near, far, arrivals):
        return call(
            lambda *refs: group_body(slots, *refs),
            [((RHS, PTS), F32), ((RHS, RANK), F32)],
            [flags, points, norm_x, z, norm_z, cols, near, far] + arrivals,
            smem=1, flops=3 * 10**9 * len(slots), far=len(arrivals),
            scratch=scratch + [pltpu.SemaphoreType.DMA],
        )

    near, far = group((1, 2, 3, 4), near, far, first_arrivals)
    near, far = group((5, 6), near, far, second_arrivals)
    out = call(
        final_body, [((RHS, PTS), F32)],
        [flags, near, far, proxy, leaf_basis, matrices[0:1], parent, parent_other], smem=1, flops=10**9,
    )[0]
    return out.T


def solution(mesh):
    return jax.shard_map(
        per_device,
        mesh=mesh,
        in_specs=(
            P("leaf", None),
            P("leaf", None),
            P("leaf", None),
            P("leaf", None, None, None),
            P(),
            P(),
            P(),
        ),
        out_specs=P("leaf", None),
        check_vma=False,
    )
```

```python
import jax
import jax.numpy as jnp
from jax import lax
from jax.experimental import pallas as pl
from jax.experimental.pallas import tpu as pltpu
from jax.sharding import PartitionSpec as P


GROUP = 8
PTS = 1024
DIM = 512
RANK = 256
RHS = 64
ROWS = PTS + 4 * RHS + RHS
SCALE = 2.0 / DIM
INTERPRET = False

BITS = 0
CORE = 0
OWNED = 8
KIND = 16
SIDE = 32
FARKIND = 33
BEYOND = 40

F32 = jnp.float32
BF16 = jnp.bfloat16
NN = (((1,), (0,)), ((), ()))
NT = (((1,), (1,)), ((), ()))


def mm(a, b, dims=NN):
    return lax.dot_general(a, b, dims, preferred_element_type=F32)


def split(a):
    high = a.astype(BF16)
    return high, (a - high.astype(F32)).astype(BF16)


def product(a, b, dims=NN):
    a_high, a_low = split(a)
    b_high, b_low = split(b)
    rows = a.shape[0]
    both = mm(jnp.concatenate([a_high, a_low], 0), b_high, dims)
    return both[:rows] + both[rows:] + mm(a_high, b_low, dims)


def row_norms(rows):
    wide = rows.astype(F32)
    high, low = split(wide * wide)
    ones = jnp.ones((8, rows.shape[1]), BF16)
    return mm(ones, high, NT) + mm(ones, low, NT)


def kern(left, right, right_norm):
    wide = left.astype(F32)
    left_norm = jnp.sum(wide * wide, axis=1, keepdims=True)
    inner = mm(left, right, NT)
    return jnp.exp(-SCALE * (left_norm + right_norm - 2.0 * inner))


def pick_matrix(picks, count):
    lanes = lax.broadcasted_iota(jnp.int32, (picks.shape[0], count), 1)
    return jnp.where(lanes == picks, 1.0, 0.0).astype(BF16)


def weighted(values, block):
    half = values.shape[0] // 2
    high, low = split(block)
    both = mm(values, high)
    return both[:half] + both[half:] + mm(values[:half], low)


def call(body, outs, args, smem=0, flops=0, far=0, scratch=()):
    near = len(args) - far
    in_specs = [
        pl.BlockSpec(memory_space=pltpu.SMEM if k < smem else pltpu.VMEM if k < near else pltpu.HBM)
        for k in range(len(args))
    ]
    size = sum(a.size * a.dtype.itemsize for a in args)
    return pl.pallas_call(
        body,
        out_shape=[jax.ShapeDtypeStruct(s, d) for s, d in outs],
        in_specs=in_specs,
        out_specs=[pl.BlockSpec(memory_space=pltpu.VMEM) for _ in outs],
        scratch_shapes=list(scratch),
        compiler_params=pltpu.CompilerParams(vmem_limit_bytes=40 << 20),
        cost_estimate=pl.CostEstimate(flops=flops, transcendentals=0, bytes_accessed=size),
        interpret=INTERPRET,
    )(*args)


def lift(values, pair):
    high, low = split(values)
    rows = values.shape[0]
    both = mm(jnp.concatenate([high, low], 0), pair[:, :RANK])
    return both[:rows] + both[rows:] + mm(high, pair[:, RANK:])


def lower(values, pair):
    high, low = split(values)
    rows = values.shape[0]
    both = mm(jnp.concatenate([high, low], 0), pair[:, :RANK], NT)
    return both[:rows] + both[rows:] + mm(high, pair[:, RANK:], NT)


def pack(values):
    high, low = split(values)
    return jnp.concatenate([high, low], 1)


def unpack(pair):
    return pair[:, :RANK].astype(F32) + pair[:, RANK:].astype(F32)


def prepare_body(x_ref, b_ref, v_ref, p_ref, w_ref):
    b_high, b_low = split(b_ref[...])
    v_high, v_low = split(v_ref[...])
    both = mm(jnp.concatenate([b_high, b_low], 0), v_high)
    w = both[:RHS] + both[RHS:] + mm(b_high, v_low)
    w_ref[...] = w
    p_ref[0:PTS, :] = x_ref[...]
    for k, part in enumerate((b_high[:, :DIM], b_low[:, :DIM], b_high[:, DIM:], b_low[:, DIM:])):
        p_ref[PTS + k * RHS : PTS + (k + 1) * RHS, :] = part
    p_ref[PTS + 4 * RHS :, :] = pack(w)


def skeleton_body(flag_ref, both_ref, col_ref, z_ref, nz_ref, nx_ref, rows_ref):
    for k in range(2):
        x = both_ref[k * ROWS : k * ROWS + PTS, :]
        z = mm(pick_matrix(col_ref[:, 8 + k : 9 + k], PTS), x).astype(BF16)
        z_ref[k] = z
        nz_ref[k] = row_norms(z)
        nx_ref[k] = row_norms(x)
    upper = flag_ref[BITS] * RANK
    picks = col_ref[:, 1:2]
    rows = mm(pick_matrix(picks - upper, RANK), z_ref[0]) + mm(pick_matrix(picks - (RANK - upper), RANK), z_ref[1])
    rows_ref[...] = rows.astype(BF16)


def add_near(source, x, norm, near_ref, place):
    p_ref, top = source

    def step(k, carry):
        for h in range(2):
            first = pl.multiple_of(top + k * 512 + h * 256, 16)
            block = kern(p_ref[pl.ds(first, 256), :], x, norm)
            row = pl.multiple_of(top + PTS + k * (2 * RHS), 16)
            values = p_ref[pl.ds(row, 2 * RHS), h * 256 : (h + 1) * 256]
            near_ref[place] += weighted(values, block)
        return carry

    lax.fori_loop(0, 2, step, 0)


def add_far(source, picks, z, norm, far_ref, place):
    p_ref, top = source
    rows = mm(pick_matrix(picks, PTS), p_ref[pl.ds(pl.multiple_of(top, 16), PTS), :]).astype(BF16)
    block = kern(rows, z, norm)
    w = p_ref[pl.ds(pl.multiple_of(top + PTS + 4 * RHS, 16), RHS), :]
    values = jnp.concatenate([w[:, :RANK], w[:, RANK:]], 0)
    far_ref[place] += weighted(values, block)


def load(source, target, semaphore):
    copy = pltpu.make_async_copy(source, target, semaphore)
    copy.start()
    copy.wait()


def self_body(flag_ref, z_ref, nz_ref, nx_ref, col_ref, both, near_ref, far_ref, own, semaphore):
    @pl.when(flag_ref[CORE] == 0)
    def _():
        load(both, own, semaphore)
        near_ref[...] = jnp.zeros_like(near_ref)
        far_ref[...] = jnp.zeros_like(far_ref)

        def leaf_terms(i, carry):
            x = own[pl.ds(pl.multiple_of(i * ROWS, 16), PTS), :]
            norm = nx_ref[i, 0:1, :]
            add_near((own, i * ROWS), x, norm, near_ref, i)
            other = (own, (1 - i) * ROWS)

            @pl.when(flag_ref[KIND + 8 * i] == 1)
            def _():
                add_near(other, x, norm, near_ref, i)

            @pl.when(flag_ref[KIND + 8 * i] == 2)
            def _():
                picks = jnp.where(i == 0, col_ref[:, 9:10], col_ref[:, 8:9])
                add_far(other, picks, z_ref[i], nz_ref[i, 0:1, :], far_ref, i)

            return carry

        lax.fori_loop(0, 2, leaf_terms, 0)


def group_body(first, flag_ref, z_ref, nz_ref, nx_ref, col_ref, near_in, far_in, both, *refs):
    arrivals = refs[:2]
    near_ref, far_ref, own, other, semaphore = refs[2:]

    def terms(slot):
        def pair_terms(n, carry):
            i, k = n >> 1, n & 1
            source = (other, k * ROWS)
            kind = flag_ref[KIND + 8 * i + slot + k]

            @pl.when(kind == 1)
            def _():
                x = own[pl.ds(pl.multiple_of(i * ROWS, 16), PTS), :]
                add_near(source, x, nx_ref[i, 0:1, :], near_ref, i)

            @pl.when(kind == 2)
            def _():
                picks = jnp.where(k == 0, col_ref[:, 9 + slot : 10 + slot], col_ref[:, 10 + slot : 11 + slot])
                add_far(source, picks, z_ref[i], nz_ref[i, 0:1, :], far_ref, i)

            return carry

        lax.fori_loop(0, 4, pair_terms, 0)

    @pl.when(flag_ref[CORE] == 0)
    def _():
        near_ref[...] = near_in[...]
        far_ref[...] = far_in[...]
        load(both, own, semaphore)
        if first:
            for k, slot in enumerate((1, 3)):

                @pl.when(flag_ref[KIND + slot] > 0)
                def _():
                    load(arrivals[k], other, semaphore)
                    terms(slot)
        else:
            for k in range(2):

                @pl.when(flag_ref[BEYOND] == 1 - k)
                def _():
                    load(arrivals[k], other, semaphore)

            terms(5)


def proxy_body(flag_ref, col_ref, right1, left1, right2, left2, out_ref, ends, other, near_ref, far_ref, z_ref, semaphore):
    @pl.when((flag_ref[CORE] == 0) & (flag_ref[SIDE] > 0))
    def _():
        near_ref[...] = jnp.zeros_like(near_ref)
        far_ref[...] = jnp.zeros_like(far_ref)

        @pl.when(flag_ref[SIDE] == 1)
        def _():
            load(right1, ends, semaphore)
            load(left2, other, semaphore)

        @pl.when(flag_ref[SIDE] == 2)
        def _():
            load(left1, ends, semaphore)
            load(right2, other, semaphore)

        def pair_terms(n, carry):
            i, k = n >> 1, n & 1
            source = (other, k * ROWS)
            kind = flag_ref[FARKIND + n]
            x = ends[pl.ds(pl.multiple_of(i * ROWS, 16), PTS), :]

            @pl.when(kind == 1)
            def _():
                add_near(source, x, row_norms(x)[0:1, :], near_ref, i)

            @pl.when(kind == 2)
            def _():
                picks = jnp.where(i == 0, col_ref[:, 16:17], col_ref[:, 17:18])
                z_ref[...] = mm(pick_matrix(picks, PTS), x).astype(BF16)
                z_norm = row_norms(z_ref[...])[0:1, :]
                far_picks = jnp.where(k == 0, col_ref[:, 14:15], col_ref[:, 15:16])
                add_far(source, far_picks, z_ref[...], z_norm, far_ref, i)

            return carry

        lax.fori_loop(0, 4, pair_terms, 0)

        out_ref[:, :, 0:PTS] = near_ref[...]
        out_ref[:, :, PTS:] = far_ref[...]


def node_body(height, last, flag_ref, col_ref, own_ref, sib_ref, *outs):
    outs = list(outs)

    @pl.when(flag_ref[CORE] == 1)
    def _():
        rest = list(outs)
        own = own_ref[...]
        sib = sib_ref[...]
        if not last:
            upper = flag_ref[BITS + height] * RANK
            picks = col_ref[:, height + 1 : height + 2]
            rows = mm(pick_matrix(picks - upper, RANK), own) + mm(pick_matrix(picks - (RANK - upper), RANK), sib)
            rest.pop(0)[...] = rows.astype(BF16)
        if height >= 3:
            rest.pop(0)[...] = kern(sib, own, row_norms(own)[0:1, :])


def mask_body(count, flag_ref, t_ref, w_ref, out_ref):
    for k in range(count):
        out_ref[k * RANK : (k + 1) * RANK, :] = pack(jnp.where(flag_ref[OWNED + k] == 1, t_ref[k + 1], 0.0))
    out_ref[count * RANK :, :] = pack(product(w_ref[...], t_ref[0]))


def sides(flag_ref, bit, size):
    upper = flag_ref[BITS + bit]
    return (
        pl.multiple_of(upper * size, 16),
        pl.multiple_of((1 - upper) * size, 16),
    )


def first_body(count, flag_ref, held_ref, arrived_ref, one_ref, two_ref, keep_ref, send_ref, lifted_ref):
    @pl.when(flag_ref[CORE] == 1)
    def _():
        one_ref[...] = held_ref[0:RANK, :] + arrived_ref[0:RANK, :]
        two = held_ref[RANK : 2 * RANK, :] + arrived_ref[RANK : 2 * RANK, :]
        two_ref[...] = two
        send_ref[0:RANK, :] = two
        keep, send = sides(flag_ref, 1, 128)
        for k in range(count - 2):
            mine = pl.ds((k + 2) * RANK + keep, 128)
            theirs = pl.ds((k + 2) * RANK + send, 128)
            keep_ref[k] = held_ref[mine, :] + arrived_ref[mine, :]
            send_ref[RANK + k * 128 : RANK + (k + 1) * 128, :] = held_ref[theirs, :] + arrived_ref[theirs, :]
        w = unpack(held_ref[count * RANK :, :]) + unpack(arrived_ref[count * RANK :, :])
        lifted = lift(w, one_ref[...])
        lifted_ref[...] = lifted
        send_ref[RANK + (count - 2) * 128 :, :] = pack(lifted)


def second_body(count, flag_ref, two_ref, held_ref, lifted_ref, arrived_ref, full_ref, keep_ref, send_ref, out_ref):
    @pl.when(flag_ref[CORE] == 1)
    def _():
        full_ref[...] = two_ref[...] + arrived_ref[0:RANK, :]
        keep, send = sides(flag_ref, 2, 64)
        for k in range(count - 2):
            top = RANK + k * 128
            keep_ref[k] = held_ref[k, pl.ds(keep, 64), :] + arrived_ref[pl.ds(top + keep, 64), :]
            send_ref[k * 64 : (k + 1) * 64, :] = held_ref[k, pl.ds(send, 64), :] + arrived_ref[pl.ds(top + send, 64), :]
        w = lifted_ref[...] + unpack(arrived_ref[RANK + (count - 2) * 128 :, :])
        lifted = lift(w, full_ref[...])
        out_ref[...] = lifted
        send_ref[(count - 2) * 64 :, :] = pack(lifted)


def third_body(count, held_ref, lifted_ref, arrived_ref, done_ref, rest_ref, w_ref):
    done_ref[...] = held_ref[0] + arrived_ref[0:64, :]
    for k in range(1, count - 2):
        rest_ref[k - 1] = held_ref[k] + arrived_ref[k * 64 : (k + 1) * 64, :]
    w_ref[...] = lifted_ref[...] + unpack(arrived_ref[(count - 2) * 64 :, :])


def add_body(held_ref, arrived_ref, done_ref, rest_ref):
    total = held_ref[...] + arrived_ref[...]
    done_ref[...] = total[0]
    rest_ref[...] = total[1:]


def gather_body(*refs):
    held_ref, arrived_ref, out_ref = refs[-3:]
    for k, ref in enumerate(refs[:-3]):
        out_ref[k] = ref[...]
    out_ref[len(refs) - 3] = held_ref[0] + arrived_ref[0]


def join_body(bit, flag_ref, held_ref, arrived_ref, *refs):
    lifting = len(refs) > 1
    out_ref = refs[-2] if lifting else refs[-1]

    @pl.when(flag_ref[CORE] == 1)
    def _():
        size = arrived_ref.shape[1]
        mine, theirs = sides(flag_ref, bit, size)
        for k in range(arrived_ref.shape[0]):
            out_ref[k, pl.ds(mine, size), :] = held_ref[k]
            out_ref[k, pl.ds(theirs, size), :] = arrived_ref[k]
        if lifting:
            w = refs[0][...]
            refs[-1][0:RHS, :] = lift(w, out_ref[0])
            refs[-1][RHS:, :] = w


def climb_body(place, lifted_ref, arrived_ref, pair_ref, out_ref):
    w = lifted_ref[0:RHS, :] + arrived_ref[0:RHS, :]
    out_ref[RHS:, :] = w
    out_ref[0:RHS, :] = lift(w, pair_ref[place])


def descend_body(levels, flag_ref, one_ref, two_ref, pairs_ref, *refs):
    out_ref = refs[-1]
    blocks = refs[0 : levels - 3]
    coeffs = refs[levels - 3 : -1]

    @pl.when(flag_ref[CORE] == 1)
    def _():
        def coupling(height):
            values = coeffs[height - 3]
            values = values[RHS:, :] if values.shape[0] > RHS else values[...]
            return product(values, blocks[height - 3][...])

        field = coupling(levels - 1)
        for height in range(levels - 2, 0, -1):
            matrix = one_ref[...] if height == 1 else two_ref[...] if height == 2 else pairs_ref[height - 3]
            field = lower(field, matrix)
            if height >= 3:
                field = field + coupling(height)
        out_ref[...] = field


def final_body(flag_ref, near_ref, far_ref, handed_ref, even_ref, odd_ref, v_ref, t_ref, held_ref, arrived_ref, out_ref):
    def finish(near, far, parent):
        field = product(parent, t_ref[0], NT) + far + even_ref[:, PTS:] + odd_ref[:, PTS:]
        out_ref[...] = near + even_ref[:, 0:PTS] + odd_ref[:, 0:PTS] + product(field, v_ref[...], NT)

    upper = flag_ref[CORE] == 1
    finish(
        jnp.where(upper, handed_ref[:, 0:PTS], near_ref[0]),
        jnp.where(upper, handed_ref[:, PTS:], far_ref[0]),
        jnp.where(upper, held_ref[...], arrived_ref[...]),
    )


def whole(points, weights, leaf_basis, transfer, skeleton_index, node_owner, near_list):
    count = lax.axis_size("leaf")
    levels = count.bit_length() - 1
    upper = levels - 2
    leaf = lax.axis_index("leaf")
    bits = [leaf >> b & 1 for b in range(levels)]
    core = bits[0]
    line = leaf >> 1 & 3
    start = leaf - leaf % GROUP
    everyone = range(count)

    def move(value, pairs):
        return lax.ppermute(value, "leaf", pairs)

    def cross(value, bit):
        return move(value, [(s, s ^ (1 << bit)) for s in everyone if s & 1])

    def shift(value, step, lines):
        return move(value, [(s, s + 2 * step) for s in everyone if s & 1 == 0 and (s >> 1 & 3) in lines])

    payload, w = call(
        prepare_body,
        [((ROWS, DIM), BF16), ((RHS, RANK), F32)],
        [points, weights.T, leaf_basis],
        flops=10**9,
    )
    partner = move(payload, [(s, s ^ 1) for s in everyone])
    both = jnp.concatenate([payload, partner], 0)
    right1 = shift(both, 1, (0, 1, 2))
    left1 = shift(both, -1, (1, 2, 3))
    right2 = shift(right1, 1, (1, 2))
    left2 = shift(left1, -1, (1, 2))

    beyond = line >= 2
    far_end = jnp.where(beyond, line - 2, line + 2)
    places = jnp.stack([line - 1, line - 1, line + 1, line + 1, far_end, far_end])
    cores = jnp.arange(6, dtype=jnp.int32) & 1
    there = (places >= 0) & (places <= 3)
    targets = jnp.where(there, places, 0) * 2 + cores
    end = start + jnp.where(line == 2, 3, 0) * 2
    works = (line == 1) | (line == 2)
    base = leaf - core
    rows = near_list.reshape(count // 2, 6)
    mine = lax.dynamic_slice(rows, (leaf >> 1, 0), (1, 6)).reshape(2, 3)
    ends_rows = lax.dynamic_slice(rows, (end >> 1, 0), (1, 6)).reshape(2, 3)

    def kinds_of(lists, first, spots, valid):
        position = (first % GROUP) + jnp.arange(2, dtype=jnp.int32)
        offsets = spots ^ position[:, None]
        listed = jnp.any(lists[:, None, :] == offsets[:, :, None], axis=2)
        return jnp.where(valid, jnp.where(listed, 1, 2), 0).astype(jnp.int32)

    other = (base % GROUP) + 1 - jnp.arange(2, dtype=jnp.int32)
    spots = jnp.concatenate([other[:, None], jnp.broadcast_to(targets, (2, 6))], 1)
    valid = jnp.concatenate([jnp.ones((1,), bool), there])
    kinds = jnp.pad(kinds_of(mine, base, spots, valid[None, :]), ((0, 0), (0, 1))).reshape(-1)
    far_kinds = kinds_of(ends_rows, end, jnp.broadcast_to(targets[4:6], (2, 2)), works).reshape(-1)
    side = jnp.where(line == 1, 1, jnp.where(line == 2, 2, 0))
    steps = jnp.arange(8, dtype=jnp.int32)
    bit_row = (leaf >> steps) & 1
    owners = jnp.pad(node_owner, ((0, 6 - node_owner.shape[0]), (0, 0))).reshape(-1)
    heights6 = jnp.arange(1, 7, dtype=jnp.int32)
    owner = jnp.take(owners, (heights6 - 1) * node_owner.shape[1] + (leaf >> heights6))
    owned = (owner == (leaf & ((1 << heights6) - 1))).astype(jnp.int32)
    flags = jnp.concatenate(
        [bit_row, owned, jnp.zeros((2,), jnp.int32), kinds, side[None], far_kinds,
         jnp.zeros((BEYOND - FARKIND - 4,), jnp.int32), beyond[None]]
    ).astype(jnp.int32)
    heights = jnp.minimum(steps, levels - 1)
    path = jnp.concatenate(
        [heights * skeleton_index.shape[1] + (leaf >> heights), leaf[None], leaf[None] ^ 1, start + targets,
         end[None], end[None] + 1]
    )
    cols = jnp.take(skeleton_index.reshape(-1, RANK), path, axis=0).T

    matrices = transfer[0]
    extra = upper - 2
    held = call(
        lambda *r: mask_body(upper, *r), [((upper * RANK + RHS, DIM), BF16)], [flags, matrices, w], smem=1,
    )[0]
    arrived = move(held, [(s, s + 1) for s in everyone if s & 1 == 0])
    one, two, keep, send, lifted = call(
        lambda *r: first_body(upper, *r),
        [((RANK, DIM), BF16), ((RANK, DIM), BF16), ((extra, 128, DIM), BF16),
         ((RANK + extra * 128 + RHS, DIM), BF16), ((RHS, RANK), F32)],
        [flags, held, arrived], smem=1,
    )
    two, keep, send, lifted = call(
        lambda *r: second_body(upper, *r),
        [((RANK, DIM), BF16), ((extra, 64, DIM), BF16), ((extra * 64 + RHS, DIM), BF16), ((RHS, RANK), F32)],
        [flags, two, keep, lifted, cross(send, 1)], smem=1,
    )
    done, keep, w3 = call(
        lambda *r: third_body(upper, *r),
        [((64, DIM), BF16), ((extra - 1, 64, DIM), BF16), ((RHS, RANK), F32)],
        [keep, lifted, cross(send, 2)],
    )
    quarters = [done]
    for bit in range(3, levels - 2):
        arrived = cross(keep, bit)
        if keep.shape[0] > 1:
            done, keep = call(
                add_body, [((64, DIM), BF16), ((keep.shape[0] - 1, 64, DIM), BF16)], [keep, arrived],
            )
            quarters.append(done)
    halves = call(gather_body, [((extra, 64, DIM), BF16)], quarters + [keep, arrived])[0]
    halves = call(
        lambda *r: join_body(2, *r), [((extra, 128, DIM), BF16)], [flags, halves, cross(halves, 2)], smem=1,
    )[0]
    pairs, lifted = call(
        lambda *r: join_body(1, *r), [((extra, RANK, DIM), BF16), ((2 * RHS, RANK), F32)],
        [flags, halves, cross(halves, 1), w3], smem=1,
    )

    z, norm_z, norm_x, rows = call(
        skeleton_body,
        [((2, RANK, DIM), BF16), ((2, 8, RANK), F32), ((2, 8, PTS), F32), ((RANK, DIM), BF16)],
        [flags, both, cols], smem=1,
    )
    blocks = []
    for height in range(1, levels):
        last = height + 1 == levels
        outs = ([] if last else [((RANK, DIM), BF16)]) + ([((RANK, RANK), F32)] if height >= 3 else [])
        result = call(
            lambda *refs: node_body(height, last, *refs),
            outs,
            [flags, cols, rows, cross(rows, height)],
            smem=1,
        )
        if height >= 3:
            blocks.append(result[-1])
        rows = result[0]

    coeffs = []
    for height in range(3, levels - 1):
        if height > 3:
            lifted = call(
                lambda *r: climb_body(height - 3, *r), [((2 * RHS, RANK), F32)], [lifted, arrived, pairs],
            )[0]
        arrived = cross(lifted, height)
        coeffs.append(arrived)
    top = lifted[:RHS] + arrived[:RHS]
    coeffs.append(cross(top, levels - 1))
    parent = call(
        lambda *refs: descend_body(levels, *refs), [((RHS, RANK), F32)],
        [flags, one, two, pairs] + blocks + coeffs, smem=1,
    )[0]
    parent_other = move(parent, [(s, s - 1) for s in everyone if s & 1])

    sums = [((2, RHS, PTS), F32), ((2, RHS, RANK), F32)]
    shared = [flags, z, norm_z, norm_x, cols]
    hold = pltpu.VMEM((2 * ROWS, DIM), BF16)
    near, far = call(
        self_body, sums, shared + [both], smem=1, far=1, scratch=[hold, pltpu.SemaphoreType.DMA], flops=5 * 10**9,
    )
    near, far = call(
        lambda *r: group_body(True, *r), sums, shared + [near, far, both, right1, left1],
        smem=1, far=3, scratch=[hold, hold, pltpu.SemaphoreType.DMA], flops=10**10,
    )
    proxy = call(
        proxy_body, [((2, RHS, PTS + RANK), F32)], [flags, cols, right1, left1, right2, left2],
        smem=1, far=4,
        scratch=[hold, hold, pltpu.VMEM((2, RHS, PTS), F32), pltpu.VMEM((2, RHS, RANK), F32),
                 pltpu.VMEM((RANK, DIM), BF16), pltpu.SemaphoreType.DMA],
        flops=5 * 10**9,
    )[0]
    workers = [s for s in everyone if s & 1 == 0 and (s >> 1 & 3) in (1, 2)]
    step = lambda s: 2 if (s >> 1 & 3) == 2 else -2
    even = move(proxy[0], [(s, s + step(s)) for s in workers])
    odd = move(proxy[1], [(s, s + step(s) + 1) for s in workers])
    near, far = call(
        lambda *r: group_body(False, *r), sums, shared + [near, far, both, right2, left2],
        smem=1, far=3, scratch=[hold, hold, pltpu.SemaphoreType.DMA], flops=5 * 10**9,
    )
    handed = move(jnp.concatenate([near[1], far[1]], 1), [(s, s + 1) for s in everyone if s & 1 == 0])
    out = call(
        final_body, [((RHS, PTS), F32)],
        [flags, near, far, handed, even, odd, leaf_basis, matrices[0:1], parent, parent_other], smem=1, flops=10**9,
    )[0]
    return out.T


def solution(mesh):
    return jax.shard_map(
        whole,
        mesh=mesh,
        in_specs=(
            P("leaf", None),
            P("leaf", None),
            P("leaf", None),
            P("leaf", None, None, None),
            P(),
            P(),
            P(),
        ),
        out_specs=P("leaf", None),
        check_vma=False,
    )
```

```python
import jax
import jax.numpy as jnp
from jax import lax
from jax.experimental import pallas as pl
from jax.experimental.pallas import tpu as pltpu
from jax.sharding import PartitionSpec as P


GROUP = 8
PTS = 1024
DIM = 512
RANK = 256
RHS = 64
ROWS = PTS + 4 * RHS + RHS
SCALE = 2.0 / DIM
INTERPRET = False

F32 = jnp.float32
BF16 = jnp.bfloat16
NN = (((1,), (0,)), ((), ()))
NT = (((1,), (1,)), ((), ()))


def mm(a, b, dims=NN):
    return lax.dot_general(a, b, dims, preferred_element_type=F32)


def split(a):
    high = a.astype(BF16)
    return high, (a - high.astype(F32)).astype(BF16)


def product(a, b, dims=NN):
    a_high, a_low = split(a)
    b_high, b_low = split(b)
    rows = a.shape[0]
    both = mm(jnp.concatenate([a_high, a_low], 0), b_high, dims)
    return both[:rows] + both[rows:] + mm(a_high, b_low, dims)


def row_norms(rows):
    wide = rows.astype(F32)
    high, low = split(wide * wide)
    ones = jnp.ones((8, rows.shape[1]), BF16)
    return mm(ones, high, NT) + mm(ones, low, NT)


def kern(left, right, right_norm):
    wide = left.astype(F32)
    left_norm = jnp.sum(wide * wide, axis=1, keepdims=True)
    inner = mm(left, right, NT)
    return jnp.exp(-SCALE * (left_norm + right_norm - 2.0 * inner))


def pick_matrix(picks, count):
    lanes = lax.broadcasted_iota(jnp.int32, (picks.shape[0], count), 1)
    return jnp.where(lanes == picks, 1.0, 0.0).astype(BF16)


def weighted(values, block):
    half = values.shape[0] // 2
    high, low = split(block)
    both = mm(values, high)
    return both[:half] + both[half:] + mm(values[:half], low)


def call(body, outs, args, smem=0, flops=0, far=0, scratch=(), hbm=False):
    near = len(args) - far
    in_specs = [
        pl.BlockSpec(memory_space=pltpu.SMEM if k < smem else pltpu.VMEM if k < near else pltpu.HBM)
        for k in range(len(args))
    ]
    size = sum(a.size * a.dtype.itemsize for a in args)
    return pl.pallas_call(
        body,
        out_shape=[jax.ShapeDtypeStruct(s, d) for s, d in outs],
        in_specs=in_specs,
        out_specs=[pl.BlockSpec(memory_space=pltpu.HBM if hbm else pltpu.VMEM) for _ in outs],
        scratch_shapes=list(scratch),
        compiler_params=pltpu.CompilerParams(vmem_limit_bytes=40 << 20),
        cost_estimate=pl.CostEstimate(flops=flops, transcendentals=0, bytes_accessed=size),
        interpret=INTERPRET,
    )(*args)


def lift(values, pair):
    high, low = split(values)
    rows = values.shape[0]
    both = mm(jnp.concatenate([high, low], 0), pair[:, :RANK])
    return both[:rows] + both[rows:] + mm(high, pair[:, RANK:])


def lower(values, pair):
    high, low = split(values)
    rows = values.shape[0]
    both = mm(jnp.concatenate([high, low], 0), pair[:, :RANK], NT)
    return both[:rows] + both[rows:] + mm(high, pair[:, RANK:], NT)


def pack(values):
    high, low = split(values)
    return jnp.concatenate([high, low], 1)


def unpack(pair):
    return pair[:, :RANK].astype(F32) + pair[:, RANK:].astype(F32)


def prepare_body(x_ref, b_ref, v_ref, p_ref, w_ref):
    b_high, b_low = split(b_ref[...])
    v_high, v_low = split(v_ref[...])
    both = mm(jnp.concatenate([b_high, b_low], 0), v_high)
    w = both[:RHS] + both[RHS:] + mm(b_high, v_low)
    w_ref[...] = w
    p_ref[0:PTS, :] = x_ref[...]
    for k, part in enumerate((b_high[:, :DIM], b_low[:, :DIM], b_high[:, DIM:], b_low[:, DIM:])):
        p_ref[PTS + k * RHS : PTS + (k + 1) * RHS, :] = part
    p_ref[PTS + 4 * RHS :, :] = pack(w)


def bit_of(leaf_ref, bit):
    return leaf_ref[0] >> bit & 1


def column(col_ref, lane):
    lanes = lax.broadcasted_iota(jnp.int32, col_ref.shape, 1)
    picked = jnp.where(lanes == lane, col_ref[...].astype(F32), 0.0)
    return jnp.sum(picked, axis=1, keepdims=True).astype(jnp.int32)


def kind_of(near_ref, leaf, other):
    offset = leaf ^ other
    listed = (near_ref[0, leaf] == offset) | (near_ref[1, leaf] == offset) | (near_ref[2, leaf] == offset)
    return jnp.where(listed, 1, 2)


def skeleton_body(x_ref, col_ref, z_ref):
    z_ref[...] = mm(pick_matrix(col_ref[:, 0:1], PTS), x_ref[...]).astype(BF16)


def add_near(source, x, norm, near_ref, place):
    p_ref, top = source

    def step(k, carry):
        for h in range(2):
            first = pl.multiple_of(top + k * 512 + h * 256, 16)
            block = kern(p_ref[pl.ds(first, 256), :], x, norm)
            row = pl.multiple_of(top + PTS + k * (2 * RHS), 16)
            values = p_ref[pl.ds(row, 2 * RHS), h * 256 : (h + 1) * 256]
            near_ref[place] += weighted(values, block)
        return carry

    lax.fori_loop(0, 2, step, 0)


def add_far(source, picks, z, norm, far_ref, place):
    p_ref, top = source
    rows = mm(pick_matrix(picks, PTS), p_ref[pl.ds(pl.multiple_of(top, 16), PTS), :]).astype(BF16)
    block = kern(rows, z, norm)
    w = p_ref[pl.ds(pl.multiple_of(top + PTS + 4 * RHS, 16), RHS), :]
    values = jnp.concatenate([w[:, :RANK], w[:, RANK:]], 0)
    far_ref[place] += weighted(values, block)


def load(source, target, semaphore):
    copy = pltpu.make_async_copy(source, target, semaphore)
    copy.start()
    copy.wait()


def stack_body(leaf_ref, first, second, out, semaphore):
    @pl.when(bit_of(leaf_ref, 0) == 0)
    def _():
        load(first, out.at[pl.ds(0, ROWS), :], semaphore)
        load(second, out.at[pl.ds(ROWS, ROWS), :], semaphore)


def self_body(leaf_ref, near_list, col_ref, both, near_ref, far_ref, z_ref, nz_ref, nx_ref, own, semaphore):
    leaf = leaf_ref[0]

    @pl.when(leaf & 1 == 0)
    def _():
        load(both, own, semaphore)
        near_ref[...] = jnp.zeros_like(near_ref)
        far_ref[...] = jnp.zeros_like(far_ref)

        def leaf_terms(i, carry):
            x = own[pl.ds(pl.multiple_of(i * ROWS, 16), PTS), :]
            norm = row_norms(x)
            z = mm(pick_matrix(column(col_ref, 8 + ((leaf + i) & 7)), PTS), x).astype(BF16)
            z_norm = row_norms(z)
            nx_ref[i] = norm
            z_ref[i] = z
            nz_ref[i] = z_norm
            add_near((own, i * ROWS), x, norm[0:1, :], near_ref, i)
            source = (own, (1 - i) * ROWS)
            other = leaf + 1 - i
            kind = kind_of(near_list, leaf + i, other)

            @pl.when(kind == 1)
            def _():
                add_near(source, x, norm[0:1, :], near_ref, i)

            @pl.when(kind == 2)
            def _():
                add_far(source, column(col_ref, 8 + (other & 7)), z, z_norm[0:1, :], far_ref, i)

            return carry

        lax.fori_loop(0, 2, leaf_terms, 0)


def group_body(first, leaf_ref, near_list, col_ref, z_ref, nz_ref, nx_ref, near_in, far_in, both, *refs):
    arrivals = refs[:2]
    near_ref, far_ref, own, arrived, semaphore = refs[2:]
    leaf = leaf_ref[0]
    line = leaf >> 1 & 3

    def terms(place):
        def pair_terms(n, carry):
            i, k = n >> 1, n & 1
            source = (arrived, k * ROWS)
            other = leaf - (leaf & 7) + 2 * place + k
            kind = kind_of(near_list, leaf + i, other)

            @pl.when(kind == 1)
            def _():
                x = own[pl.ds(pl.multiple_of(i * ROWS, 16), PTS), :]
                add_near(source, x, nx_ref[i, 0:1, :], near_ref, i)

            @pl.when(kind == 2)
            def _():
                add_far(source, column(col_ref, 8 + (other & 7)), z_ref[i], nz_ref[i, 0:1, :], far_ref, i)

            return carry

        lax.fori_loop(0, 4, pair_terms, 0)

    @pl.when(leaf & 1 == 0)
    def _():
        near_ref[...] = near_in[...]
        far_ref[...] = far_in[...]
        load(both, own, semaphore)
        if first:

            @pl.when(line > 0)
            def _():
                load(arrivals[0], arrived, semaphore)
                terms(line - 1)

            @pl.when(line < 3)
            def _():
                load(arrivals[1], arrived, semaphore)
                terms(line + 1)
        else:

            @pl.when(line >= 2)
            def _():
                load(arrivals[0], arrived, semaphore)

            @pl.when(line < 2)
            def _():
                load(arrivals[1], arrived, semaphore)

            terms(jnp.where(line >= 2, line - 2, line + 2))


def proxy_body(leaf_ref, near_list, col_ref, right1, left1, right2, left2,
               out_ref, ends, arrived, near_ref, far_ref, z_ref, semaphore):
    leaf = leaf_ref[0]
    line = leaf >> 1 & 3
    start = leaf - (leaf & 7)

    @pl.when((leaf & 1 == 0) & ((line == 1) | (line == 2)))
    def _():
        near_ref[...] = jnp.zeros_like(near_ref)
        far_ref[...] = jnp.zeros_like(far_ref)

        @pl.when(line == 1)
        def _():
            load(right1, ends, semaphore)
            load(left2, arrived, semaphore)

        @pl.when(line == 2)
        def _():
            load(left1, ends, semaphore)
            load(right2, arrived, semaphore)

        client = start + jnp.where(line == 1, 0, 6)
        distant = start + jnp.where(line == 1, 6, 0)

        def pair_terms(n, carry):
            i, k = n >> 1, n & 1
            source = (arrived, k * ROWS)
            kind = kind_of(near_list, client + i, distant + k)
            x = ends[pl.ds(pl.multiple_of(i * ROWS, 16), PTS), :]

            @pl.when(kind == 1)
            def _():
                add_near(source, x, row_norms(x)[0:1, :], near_ref, i)

            @pl.when(kind == 2)
            def _():
                z_ref[...] = mm(pick_matrix(column(col_ref, 8 + ((client + i) & 7)), PTS), x).astype(BF16)
                z_norm = row_norms(z_ref[...])[0:1, :]
                add_far(source, column(col_ref, 8 + ((distant + k) & 7)), z_ref[...], z_norm, far_ref, i)

            return carry

        lax.fori_loop(0, 4, pair_terms, 0)
        out_ref[:, :, 0:PTS] = near_ref[...]
        out_ref[:, :, PTS:] = far_ref[...]


def node_body(height, last, flag_ref, col_ref, own_ref, sib_ref, *outs):
    outs = list(outs)

    @pl.when(bit_of(flag_ref, 0) == 1)
    def _():
        rest = list(outs)
        own = own_ref[...]
        sib = sib_ref[...]
        if not last:
            upper = bit_of(flag_ref, height) * RANK
            picks = col_ref[:, height + 1 : height + 2]
            rows = mm(pick_matrix(picks - upper, RANK), own) + mm(pick_matrix(picks - (RANK - upper), RANK), sib)
            rest.pop(0)[...] = rows.astype(BF16)
        if height >= 3:
            rest.pop(0)[...] = kern(sib, own, row_norms(own)[0:1, :])


def mask_body(count, leaf_ref, owner_ref, t_ref, w_ref, out_ref, leaf_pair_ref):
    leaf = leaf_ref[0]
    for k in range(count):
        mine = owner_ref[k, leaf >> (k + 1)] == leaf & ((2 << k) - 1)
        out_ref[k * RANK : (k + 1) * RANK, :] = pack(jnp.where(mine, t_ref[k + 1], 0.0))
    pair = pack(t_ref[0])
    leaf_pair_ref[...] = pair
    out_ref[count * RANK :, :] = pack(lift(w_ref[...], pair))


def sides(flag_ref, bit, size):
    upper = bit_of(flag_ref, bit)
    return (
        pl.multiple_of(upper * size, 16),
        pl.multiple_of((1 - upper) * size, 16),
    )


def first_body(count, flag_ref, held_ref, arrived_ref, one_ref, two_ref, keep_ref, send_ref, lifted_ref):
    @pl.when(bit_of(flag_ref, 0) == 1)
    def _():
        one_ref[...] = held_ref[0:RANK, :] + arrived_ref[0:RANK, :]
        two = held_ref[RANK : 2 * RANK, :] + arrived_ref[RANK : 2 * RANK, :]
        two_ref[...] = two
        send_ref[0:RANK, :] = two
        keep, send = sides(flag_ref, 1, 128)
        for k in range(count - 2):
            mine = pl.ds((k + 2) * RANK + keep, 128)
            theirs = pl.ds((k + 2) * RANK + send, 128)
            keep_ref[k] = held_ref[mine, :] + arrived_ref[mine, :]
            send_ref[RANK + k * 128 : RANK + (k + 1) * 128, :] = held_ref[theirs, :] + arrived_ref[theirs, :]
        w = unpack(held_ref[count * RANK :, :]) + unpack(arrived_ref[count * RANK :, :])
        lifted = lift(w, one_ref[...])
        lifted_ref[...] = lifted
        send_ref[RANK + (count - 2) * 128 :, :] = pack(lifted)


def second_body(count, flag_ref, two_ref, held_ref, lifted_ref, arrived_ref, full_ref, keep_ref, send_ref, out_ref):
    @pl.when(bit_of(flag_ref, 0) == 1)
    def _():
        full_ref[...] = two_ref[...] + arrived_ref[0:RANK, :]
        keep, send = sides(flag_ref, 2, 64)
        for k in range(count - 2):
            top = RANK + k * 128
            keep_ref[k] = held_ref[k, pl.ds(keep, 64), :] + arrived_ref[pl.ds(top + keep, 64), :]
            send_ref[k * 64 : (k + 1) * 64, :] = held_ref[k, pl.ds(send, 64), :] + arrived_ref[pl.ds(top + send, 64), :]
        w = lifted_ref[...] + unpack(arrived_ref[RANK + (count - 2) * 128 :, :])
        lifted = lift(w, full_ref[...])
        out_ref[...] = lifted
        send_ref[(count - 2) * 64 :, :] = pack(lifted)


def third_body(count, held_ref, lifted_ref, arrived_ref, done_ref, rest_ref, w_ref):
    done_ref[...] = held_ref[0] + arrived_ref[0:64, :]
    for k in range(1, count - 2):
        rest_ref[k - 1] = held_ref[k] + arrived_ref[k * 64 : (k + 1) * 64, :]
    w_ref[...] = lifted_ref[...] + unpack(arrived_ref[(count - 2) * 64 :, :])


def add_body(held_ref, arrived_ref, done_ref, rest_ref):
    total = held_ref[...] + arrived_ref[...]
    done_ref[...] = total[0]
    rest_ref[...] = total[1:]


def gather_body(*refs):
    held_ref, arrived_ref, out_ref = refs[-3:]
    for k, ref in enumerate(refs[:-3]):
        out_ref[k] = ref[...]
    out_ref[len(refs) - 3] = held_ref[0] + arrived_ref[0]


def join_body(bit, flag_ref, held_ref, arrived_ref, *refs):
    lifting = len(refs) > 1
    out_ref = refs[-2] if lifting else refs[-1]

    @pl.when(bit_of(flag_ref, 0) == 1)
    def _():
        size = arrived_ref.shape[1]
        mine, theirs = sides(flag_ref, bit, size)
        for k in range(arrived_ref.shape[0]):
            out_ref[k, pl.ds(mine, size), :] = held_ref[k]
            out_ref[k, pl.ds(theirs, size), :] = arrived_ref[k]
        if lifting:
            w = refs[0][...]
            refs[-1][0:RHS, :] = lift(w, out_ref[0])
            refs[-1][RHS:, :] = w


def climb_body(place, lifted_ref, arrived_ref, pair_ref, out_ref):
    w = lifted_ref[0:RHS, :] + arrived_ref[0:RHS, :]
    out_ref[RHS:, :] = w
    out_ref[0:RHS, :] = lift(w, pair_ref[place])


def descend_body(levels, flag_ref, one_ref, two_ref, pairs_ref, *refs):
    out_ref = refs[-1]
    blocks = refs[0 : levels - 3]
    coeffs = refs[levels - 3 : -1]

    @pl.when(bit_of(flag_ref, 0) == 1)
    def _():
        def coupling(height):
            values = coeffs[height - 3]
            values = values[RHS:, :] if values.shape[0] > RHS else values[...]
            return product(values, blocks[height - 3][...])

        field = coupling(levels - 1)
        for height in range(levels - 2, 0, -1):
            matrix = one_ref[...] if height == 1 else two_ref[...] if height == 2 else pairs_ref[height - 3]
            field = lower(field, matrix)
            if height >= 3:
                field = field + coupling(height)
        out_ref[...] = field


def final_body(flag_ref, near_ref, far_ref, handed_ref, even_ref, odd_ref, v_ref, t_ref, held_ref, arrived_ref, out_ref):
    def finish(near, far, parent):
        field = lower(parent, t_ref[...]) + far + even_ref[:, PTS:] + odd_ref[:, PTS:]
        out_ref[...] = near + even_ref[:, 0:PTS] + odd_ref[:, 0:PTS] + product(field, v_ref[...], NT)

    upper = bit_of(flag_ref, 0) == 1
    finish(
        jnp.where(upper, handed_ref[:, 0:PTS], near_ref[0]),
        jnp.where(upper, handed_ref[:, PTS:], far_ref[0]),
        jnp.where(upper, held_ref[...], arrived_ref[...]),
    )


def whole(points, weights, leaf_basis, transfer, skeleton_index, node_owner, near_list):
    count = lax.axis_size("leaf")
    levels = count.bit_length() - 1
    upper = levels - 2
    leaf = lax.axis_index("leaf")
    everyone = range(count)

    def move(value, pairs):
        return lax.ppermute(value, "leaf", pairs)

    def cross(value, bit):
        return move(value, [(s, s ^ (1 << bit)) for s in everyone if s & 1])

    def to_tree(value):
        return move(value, [(s, s + 1) for s in everyone if s & 1 == 0])

    def shift(value, step, lines):
        return move(value, [(s, s + 2 * step) for s in everyone if s & 1 == 0 and (s >> 1 & 3) in lines])

    place = leaf.astype(jnp.int32)[None]
    near_rows = near_list.T
    columns = jnp.arange(16, dtype=jnp.int32)
    heights = jnp.minimum(columns, levels - 1)
    path = jnp.where(
        columns < 8, heights * skeleton_index.shape[1] + (leaf >> heights), leaf - leaf % GROUP + columns - 8
    )
    cols = skeleton_index.reshape(-1, RANK).at[path].get(mode="promise_in_bounds").T

    payload, w = call(
        prepare_body,
        [((ROWS, DIM), BF16), ((RHS, RANK), F32)],
        [points, weights.T, leaf_basis],
        flops=10**9,
    )
    partner = move(payload, [(s, s ^ 1) for s in everyone])
    both = call(
        stack_body, [((2 * ROWS, DIM), BF16)], [place, payload, partner], smem=1, far=2,
        scratch=[pltpu.SemaphoreType.DMA], hbm=True,
    )[0]
    right1 = shift(both, 1, (0, 1, 2))
    left1 = shift(both, -1, (1, 2, 3))
    right2 = shift(right1, 1, (1, 2))
    left2 = shift(left1, -1, (1, 2))

    matrices = transfer[0]
    extra = upper - 2
    held, leaf_pair = call(
        lambda *r: mask_body(upper, *r), [((upper * RANK + RHS, DIM), BF16), ((RANK, DIM), BF16)],
        [place, node_owner, matrices, w], smem=2,
    )
    arrived = to_tree(held)
    one, two, keep, send, lifted = call(
        lambda *r: first_body(upper, *r),
        [((RANK, DIM), BF16), ((RANK, DIM), BF16), ((extra, 128, DIM), BF16),
         ((RANK + extra * 128 + RHS, DIM), BF16), ((RHS, RANK), F32)],
        [place, held, arrived], smem=1,
    )
    two, keep, send, lifted = call(
        lambda *r: second_body(upper, *r),
        [((RANK, DIM), BF16), ((extra, 64, DIM), BF16), ((extra * 64 + RHS, DIM), BF16), ((RHS, RANK), F32)],
        [place, two, keep, lifted, cross(send, 1)], smem=1,
    )
    done, keep, w3 = call(
        lambda *r: third_body(upper, *r),
        [((64, DIM), BF16), ((extra - 1, 64, DIM), BF16), ((RHS, RANK), F32)],
        [keep, lifted, cross(send, 2)],
    )
    quarters = [done]
    for bit in range(3, levels - 2):
        arrived = cross(keep, bit)
        if keep.shape[0] > 1:
            done, keep = call(
                add_body, [((64, DIM), BF16), ((keep.shape[0] - 1, 64, DIM), BF16)], [keep, arrived],
            )
            quarters.append(done)
    halves = call(gather_body, [((extra, 64, DIM), BF16)], quarters + [keep, arrived])[0]
    halves = call(
        lambda *r: join_body(2, *r), [((extra, 128, DIM), BF16)], [place, halves, cross(halves, 2)], smem=1,
    )[0]
    pairs, lifted = call(
        lambda *r: join_body(1, *r), [((extra, RANK, DIM), BF16), ((2 * RHS, RANK), F32)],
        [place, halves, cross(halves, 1), w3], smem=1,
    )

    rows = call(skeleton_body, [((RANK, DIM), BF16)], [points, cols])[0]
    blocks = []
    for height in range(levels):
        last = height + 1 == levels
        outs = ([] if last else [((RANK, DIM), BF16)]) + ([((RANK, RANK), F32)] if height >= 3 else [])
        result = call(
            lambda *refs: node_body(height, last, *refs),
            outs,
            [place, cols, rows, cross(rows, height) if height else to_tree(rows)],
            smem=1,
        )
        if height >= 3:
            blocks.append(result[-1])
        rows = result[0]

    coeffs = []
    for height in range(3, levels - 1):
        if height > 3:
            lifted = call(
                lambda *r: climb_body(height - 3, *r), [((2 * RHS, RANK), F32)], [lifted, arrived, pairs],
            )[0]
        arrived = cross(lifted, height)
        coeffs.append(arrived)
    top = lifted[:RHS] + arrived[:RHS]
    coeffs.append(cross(top, levels - 1))
    parent = call(
        lambda *refs: descend_body(levels, *refs), [((RHS, RANK), F32)],
        [place, one, two, pairs] + blocks + coeffs, smem=1,
    )[0]
    parent_other = move(parent, [(s, s - 1) for s in everyone if s & 1])

    sums = [((2, RHS, PTS), F32), ((2, RHS, RANK), F32)]
    shared = [place, near_rows, cols]
    hold = pltpu.VMEM((2 * ROWS, DIM), BF16)
    near, far, z, norm_z, norm_x = call(
        self_body, sums + [((2, RANK, DIM), BF16), ((2, 8, RANK), F32), ((2, 8, PTS), F32)], shared + [both],
        smem=2, far=1, scratch=[hold, pltpu.SemaphoreType.DMA], flops=5 * 10**9,
    )
    near, far = call(
        lambda *r: group_body(True, *r), sums, shared + [z, norm_z, norm_x, near, far, both, right1, left1],
        smem=2, far=3, scratch=[hold, hold, pltpu.SemaphoreType.DMA], flops=10**10,
    )
    proxy = call(
        proxy_body, [((2, RHS, PTS + RANK), F32)], shared + [right1, left1, right2, left2],
        smem=2, far=4,
        scratch=[hold, hold, pltpu.VMEM((2, RHS, PTS), F32), pltpu.VMEM((2, RHS, RANK), F32),
                 pltpu.VMEM((RANK, DIM), BF16), pltpu.SemaphoreType.DMA],
        flops=5 * 10**9,
    )[0]
    workers = [s for s in everyone if s & 1 == 0 and (s >> 1 & 3) in (1, 2)]
    step = lambda s: 2 if (s >> 1 & 3) == 2 else -2
    even = move(proxy[0], [(s, s + step(s)) for s in workers])
    odd = move(proxy[1], [(s, s + step(s) + 1) for s in workers])
    near, far = call(
        lambda *r: group_body(False, *r), sums, shared + [z, norm_z, norm_x, near, far, both, right2, left2],
        smem=2, far=3, scratch=[hold, hold, pltpu.SemaphoreType.DMA], flops=5 * 10**9,
    )
    handed = move(jnp.concatenate([near[1], far[1]], 1), [(s, s + 1) for s in everyone if s & 1 == 0])
    out = call(
        final_body, [((RHS, PTS), F32)],
        [place, near, far, handed, even, odd, leaf_basis, leaf_pair, parent, parent_other], smem=1, flops=10**9,
    )[0]
    return out.T


def solution(mesh):
    return jax.shard_map(
        whole,
        mesh=mesh,
        in_specs=(
            P("leaf", None),
            P("leaf", None),
            P("leaf", None),
            P("leaf", None, None, None),
            P(),
            P(),
            P(),
        ),
        out_specs=P("leaf", None),
        check_vma=False,
    )
```

```python
import jax
import jax.numpy as jnp
from jax import lax
from jax.experimental import pallas as pl
from jax.experimental.pallas import tpu as pltpu
from jax.sharding import PartitionSpec as P


GROUP = 8
PTS = 1024
DIM = 512
RANK = 256
RHS = 64
ROWS = PTS + 4 * RHS + RHS
SCALE = 2.0 / DIM
INTERPRET = False

F32 = jnp.float32
BF16 = jnp.bfloat16
NN = (((1,), (0,)), ((), ()))
NT = (((1,), (1,)), ((), ()))


def mm(a, b, dims=NN):
    return lax.dot_general(a, b, dims, preferred_element_type=F32)


def split(a):
    high = a.astype(BF16)
    return high, (a - high.astype(F32)).astype(BF16)


def product(a, b, dims=NN):
    a_high, a_low = split(a)
    b_high, b_low = split(b)
    rows = a.shape[0]
    both = mm(jnp.concatenate([a_high, a_low], 0), b_high, dims)
    return both[:rows] + both[rows:] + mm(a_high, b_low, dims)


def row_norms(rows):
    wide = rows.astype(F32)
    high, low = split(wide * wide)
    ones = jnp.ones((8, rows.shape[1]), BF16)
    return mm(ones, high, NT) + mm(ones, low, NT)


def kern(left, right, right_norm):
    wide = left.astype(F32)
    left_norm = jnp.sum(wide * wide, axis=1, keepdims=True)
    inner = mm(left, right, NT)
    return jnp.exp(-SCALE * (left_norm + right_norm - 2.0 * inner))


def pick_matrix(picks, count):
    lanes = lax.broadcasted_iota(jnp.int32, (picks.shape[0], count), 1)
    return jnp.where(lanes == picks, 1.0, 0.0).astype(BF16)


def weighted(values, block):
    half = values.shape[0] // 2
    high, low = split(block)
    both = mm(values, high)
    return both[:half] + both[half:] + mm(values[:half], low)


def call(body, outs, args, smem=0, flops=0, scratch=()):
    in_specs = [
        pl.BlockSpec(memory_space=pltpu.SMEM if k < smem else pltpu.VMEM)
        for k in range(len(args))
    ]
    size = sum(a.size * a.dtype.itemsize for a in args)
    return pl.pallas_call(
        body,
        out_shape=[jax.ShapeDtypeStruct(s, d) for s, d in outs],
        in_specs=in_specs,
        out_specs=[pl.BlockSpec(memory_space=pltpu.VMEM) for _ in outs],
        scratch_shapes=list(scratch),
        compiler_params=pltpu.CompilerParams(vmem_limit_bytes=24 << 20),
        cost_estimate=pl.CostEstimate(flops=flops, transcendentals=0, bytes_accessed=size),
        interpret=INTERPRET,
    )(*args)


def lift(values, pair):
    high, low = split(values)
    rows = values.shape[0]
    both = mm(jnp.concatenate([high, low], 0), pair[:, :RANK])
    return both[:rows] + both[rows:] + mm(high, pair[:, RANK:])


def lower(values, pair):
    high, low = split(values)
    rows = values.shape[0]
    both = mm(jnp.concatenate([high, low], 0), pair[:, :RANK], NT)
    return both[:rows] + both[rows:] + mm(high, pair[:, RANK:], NT)


def pack(values):
    high, low = split(values)
    return jnp.concatenate([high, low], 1)


def unpack(pair):
    return pair[:, :RANK].astype(F32) + pair[:, RANK:].astype(F32)


def prepare_body(x_ref, b_ref, v_ref, p_ref, w_ref):
    b_high, b_low = split(b_ref[...])
    v_high, v_low = split(v_ref[...])
    both = mm(jnp.concatenate([b_high, b_low], 0), v_high)
    w = both[:RHS] + both[RHS:] + mm(b_high, v_low)
    w_ref[...] = w
    p_ref[0:PTS, :] = x_ref[...]
    for k, part in enumerate((b_high[:, :DIM], b_low[:, :DIM], b_high[:, DIM:], b_low[:, DIM:])):
        p_ref[PTS + k * RHS : PTS + (k + 1) * RHS, :] = part
    p_ref[PTS + 4 * RHS :, :] = pack(w)


def bit_of(leaf_ref, bit):
    return leaf_ref[0] >> bit & 1


def column(col_ref, lane):
    lanes = lax.broadcasted_iota(jnp.int32, col_ref.shape, 1)
    picked = jnp.where(lanes == lane, col_ref[...].astype(F32), 0.0)
    return jnp.sum(picked, axis=1, keepdims=True).astype(jnp.int32)


def kind_of(near_ref, leaf, other):
    offset = leaf ^ other
    listed = (near_ref[0, leaf] == offset) | (near_ref[1, leaf] == offset) | (near_ref[2, leaf] == offset)
    return jnp.where(listed, 1, 2)


def skeleton_body(x_ref, col_ref, z_ref):
    z_ref[...] = mm(pick_matrix(col_ref[:, 0:1], PTS), x_ref[...]).astype(BF16)


def add_near(source, x, norm, near_ref, place):
    p_ref, top = source

    def step(k, carry):
        for h in range(2):
            first = pl.multiple_of(top + k * 512 + h * 256, 16)
            block = kern(p_ref[pl.ds(first, 256), :], x, norm)
            row = pl.multiple_of(top + PTS + k * (2 * RHS), 16)
            values = p_ref[pl.ds(row, 2 * RHS), h * 256 : (h + 1) * 256]
            near_ref[place] += weighted(values, block)
        return carry

    lax.fori_loop(0, 2, step, 0)


def add_far(source, picks, z, norm, far_ref, place):
    p_ref, top = source
    rows = mm(pick_matrix(picks, PTS), p_ref[pl.ds(pl.multiple_of(top, 16), PTS), :]).astype(BF16)
    block = kern(rows, z, norm)
    w = p_ref[pl.ds(pl.multiple_of(top + PTS + 4 * RHS, 16), RHS), :]
    values = jnp.concatenate([w[:, :RANK], w[:, RANK:]], 0)
    far_ref[place] += weighted(values, block)


def stack_body(leaf_ref, first, second, out):
    @pl.when(bit_of(leaf_ref, 0) == 0)
    def _():
        out[0:ROWS, :] = first[...]
        out[ROWS:, :] = second[...]


def self_body(leaf_ref, near_list, col_ref, own, near_ref, far_ref, z_ref, nz_ref, nx_ref):
    leaf = leaf_ref[0]

    @pl.when(leaf & 1 == 0)
    def _():
        near_ref[...] = jnp.zeros_like(near_ref)
        far_ref[...] = jnp.zeros_like(far_ref)

        def leaf_terms(i, carry):
            x = own[pl.ds(pl.multiple_of(i * ROWS, 16), PTS), :]
            norm = row_norms(x)
            z = mm(pick_matrix(column(col_ref, 8 + ((leaf + i) & 7)), PTS), x).astype(BF16)
            z_norm = row_norms(z)
            nx_ref[i] = norm
            z_ref[i] = z
            nz_ref[i] = z_norm
            add_near((own, i * ROWS), x, norm[0:1, :], near_ref, i)
            source = (own, (1 - i) * ROWS)
            other = leaf + 1 - i
            kind = kind_of(near_list, leaf + i, other)

            @pl.when(kind == 1)
            def _():
                add_near(source, x, norm[0:1, :], near_ref, i)

            @pl.when(kind == 2)
            def _():
                add_far(source, column(col_ref, 8 + (other & 7)), z, z_norm[0:1, :], far_ref, i)

            return carry

        lax.fori_loop(0, 2, leaf_terms, 0)


def group_body(first, leaf_ref, near_list, col_ref, z_ref, nz_ref, nx_ref, near_in, far_in, own,
               from_left, from_right, near_ref, far_ref):
    leaf = leaf_ref[0]
    line = leaf >> 1 & 3

    def terms(place, arrived):
        def pair_terms(n, carry):
            i, k = n >> 1, n & 1
            source = (arrived, k * ROWS)
            other = leaf - (leaf & 7) + 2 * place + k
            kind = kind_of(near_list, leaf + i, other)

            @pl.when(kind == 1)
            def _():
                x = own[pl.ds(pl.multiple_of(i * ROWS, 16), PTS), :]
                add_near(source, x, nx_ref[i, 0:1, :], near_ref, i)

            @pl.when(kind == 2)
            def _():
                add_far(source, column(col_ref, 8 + (other & 7)), z_ref[i], nz_ref[i, 0:1, :], far_ref, i)

            return carry

        lax.fori_loop(0, 4, pair_terms, 0)

    @pl.when(leaf & 1 == 0)
    def _():
        near_ref[...] = near_in[...]
        far_ref[...] = far_in[...]

        @pl.when(line > 0 if first else line >= 2)
        def _():
            terms(line - (1 if first else 2), from_left)

        @pl.when(line < 3 if first else line < 2)
        def _():
            terms(line + (1 if first else 2), from_right)


def proxy_body(leaf_ref, near_list, col_ref, right1, left1, right2, left2,
               out_ref, near_ref, far_ref, z_ref):
    leaf = leaf_ref[0]
    line = leaf >> 1 & 3
    start = leaf - (leaf & 7)

    def terms(ends, arrived, client, distant):
        near_ref[...] = jnp.zeros_like(near_ref)
        far_ref[...] = jnp.zeros_like(far_ref)

        def pair_terms(n, carry):
            i, k = n >> 1, n & 1
            source = (arrived, k * ROWS)
            kind = kind_of(near_list, client + i, distant + k)
            x = ends[pl.ds(pl.multiple_of(i * ROWS, 16), PTS), :]

            @pl.when(kind == 1)
            def _():
                add_near(source, x, row_norms(x)[0:1, :], near_ref, i)

            @pl.when(kind == 2)
            def _():
                z_ref[...] = mm(pick_matrix(column(col_ref, 8 + ((client + i) & 7)), PTS), x).astype(BF16)
                z_norm = row_norms(z_ref[...])[0:1, :]
                add_far(source, column(col_ref, 8 + ((distant + k) & 7)), z_ref[...], z_norm, far_ref, i)

            return carry

        lax.fori_loop(0, 4, pair_terms, 0)
        out_ref[:, :, 0:PTS] = near_ref[...]
        out_ref[:, :, PTS:] = far_ref[...]

    @pl.when((leaf & 1 == 0) & (line == 1))
    def _():
        terms(right1, left2, start, start + 6)

    @pl.when((leaf & 1 == 0) & (line == 2))
    def _():
        terms(left1, right2, start + 6, start)


def node_body(height, last, flag_ref, col_ref, own_ref, sib_ref, *outs):
    outs = list(outs)

    @pl.when(bit_of(flag_ref, 0) == 1)
    def _():
        rest = list(outs)
        own = own_ref[...]
        sib = sib_ref[...]
        if not last:
            upper = bit_of(flag_ref, height) * RANK
            picks = col_ref[:, height + 1 : height + 2]
            rows = mm(pick_matrix(picks - upper, RANK), own) + mm(pick_matrix(picks - (RANK - upper), RANK), sib)
            rest.pop(0)[...] = rows.astype(BF16)
        if height >= 3:
            rest.pop(0)[...] = kern(sib, own, row_norms(own)[0:1, :])


def mask_body(count, leaf_ref, owner_ref, t_ref, w_ref, out_ref, leaf_pair_ref):
    leaf = leaf_ref[0]
    for k in range(count):
        mine = owner_ref[k, leaf >> (k + 1)] == leaf & ((2 << k) - 1)
        out_ref[k * RANK : (k + 1) * RANK, :] = pack(jnp.where(mine, t_ref[k + 1], 0.0))
    pair = pack(t_ref[0])
    leaf_pair_ref[...] = pair
    out_ref[count * RANK :, :] = pack(lift(w_ref[...], pair))


def sides(flag_ref, bit, size):
    upper = bit_of(flag_ref, bit)
    return (
        pl.multiple_of(upper * size, 16),
        pl.multiple_of((1 - upper) * size, 16),
    )


def first_body(count, flag_ref, held_ref, arrived_ref, one_ref, two_ref, keep_ref, send_ref, lifted_ref):
    @pl.when(bit_of(flag_ref, 0) == 1)
    def _():
        one_ref[...] = held_ref[0:RANK, :] + arrived_ref[0:RANK, :]
        two = held_ref[RANK : 2 * RANK, :] + arrived_ref[RANK : 2 * RANK, :]
        two_ref[...] = two
        send_ref[0:RANK, :] = two
        keep, send = sides(flag_ref, 1, 128)
        for k in range(count - 2):
            mine = pl.ds((k + 2) * RANK + keep, 128)
            theirs = pl.ds((k + 2) * RANK + send, 128)
            keep_ref[k] = held_ref[mine, :] + arrived_ref[mine, :]
            send_ref[RANK + k * 128 : RANK + (k + 1) * 128, :] = held_ref[theirs, :] + arrived_ref[theirs, :]
        w = unpack(held_ref[count * RANK :, :]) + unpack(arrived_ref[count * RANK :, :])
        lifted = lift(w, one_ref[...])
        lifted_ref[...] = lifted
        send_ref[RANK + (count - 2) * 128 :, :] = pack(lifted)


def second_body(count, flag_ref, two_ref, held_ref, lifted_ref, arrived_ref, full_ref, keep_ref, send_ref, out_ref):
    @pl.when(bit_of(flag_ref, 0) == 1)
    def _():
        full_ref[...] = two_ref[...] + arrived_ref[0:RANK, :]
        keep, send = sides(flag_ref, 2, 64)
        for k in range(count - 2):
            top = RANK + k * 128
            keep_ref[k] = held_ref[k, pl.ds(keep, 64), :] + arrived_ref[pl.ds(top + keep, 64), :]
            send_ref[k * 64 : (k + 1) * 64, :] = held_ref[k, pl.ds(send, 64), :] + arrived_ref[pl.ds(top + send, 64), :]
        w = lifted_ref[...] + unpack(arrived_ref[RANK + (count - 2) * 128 :, :])
        lifted = lift(w, full_ref[...])
        out_ref[...] = lifted
        send_ref[(count - 2) * 64 :, :] = pack(lifted)


def third_body(count, held_ref, lifted_ref, arrived_ref, done_ref, rest_ref, w_ref):
    done_ref[...] = held_ref[0] + arrived_ref[0:64, :]
    for k in range(1, count - 2):
        rest_ref[k - 1] = held_ref[k] + arrived_ref[k * 64 : (k + 1) * 64, :]
    w_ref[...] = lifted_ref[...] + unpack(arrived_ref[(count - 2) * 64 :, :])


def add_body(held_ref, arrived_ref, done_ref, rest_ref):
    total = held_ref[...] + arrived_ref[...]
    done_ref[...] = total[0]
    rest_ref[...] = total[1:]


def gather_body(*refs):
    held_ref, arrived_ref, out_ref = refs[-3:]
    for k, ref in enumerate(refs[:-3]):
        out_ref[k] = ref[...]
    out_ref[len(refs) - 3] = held_ref[0] + arrived_ref[0]


def join_body(bit, flag_ref, held_ref, arrived_ref, *refs):
    lifting = len(refs) > 1
    out_ref = refs[-2] if lifting else refs[-1]

    @pl.when(bit_of(flag_ref, 0) == 1)
    def _():
        size = arrived_ref.shape[1]
        mine, theirs = sides(flag_ref, bit, size)
        for k in range(arrived_ref.shape[0]):
            out_ref[k, pl.ds(mine, size), :] = held_ref[k]
            out_ref[k, pl.ds(theirs, size), :] = arrived_ref[k]
        if lifting:
            w = refs[0][...]
            refs[-1][0:RHS, :] = lift(w, out_ref[0])
            refs[-1][RHS:, :] = w


def climb_body(place, lifted_ref, arrived_ref, pair_ref, out_ref):
    w = lifted_ref[0:RHS, :] + arrived_ref[0:RHS, :]
    out_ref[RHS:, :] = w
    out_ref[0:RHS, :] = lift(w, pair_ref[place])


def descend_body(levels, flag_ref, one_ref, two_ref, pairs_ref, *refs):
    out_ref = refs[-1]
    blocks = refs[0 : levels - 3]
    coeffs = refs[levels - 3 : -1]

    @pl.when(bit_of(flag_ref, 0) == 1)
    def _():
        def coupling(height):
            values = coeffs[height - 3]
            values = values[RHS:, :] if values.shape[0] > RHS else values[...]
            return product(values, blocks[height - 3][...])

        field = coupling(levels - 1)
        for height in range(levels - 2, 0, -1):
            matrix = one_ref[...] if height == 1 else two_ref[...] if height == 2 else pairs_ref[height - 3]
            field = lower(field, matrix)
            if height >= 3:
                field = field + coupling(height)
        out_ref[...] = field


def final_body(flag_ref, near_ref, far_ref, handed_ref, even_ref, odd_ref, v_ref, t_ref, held_ref, arrived_ref, out_ref):
    def finish(near, far, parent):
        field = lower(parent, t_ref[...]) + far + even_ref[:, PTS:] + odd_ref[:, PTS:]
        out_ref[...] = near + even_ref[:, 0:PTS] + odd_ref[:, 0:PTS] + product(field, v_ref[...], NT)

    upper = bit_of(flag_ref, 0) == 1
    finish(
        jnp.where(upper, handed_ref[:, 0:PTS], near_ref[0]),
        jnp.where(upper, handed_ref[:, PTS:], far_ref[0]),
        jnp.where(upper, held_ref[...], arrived_ref[...]),
    )


def whole(points, weights, leaf_basis, transfer, skeleton_index, node_owner, near_list):
    count = lax.axis_size("leaf")
    levels = count.bit_length() - 1
    upper = levels - 2
    leaf = lax.axis_index("leaf")
    everyone = range(count)

    def move(value, pairs):
        return lax.ppermute(value, "leaf", pairs)

    def cross(value, bit):
        return move(value, [(s, s ^ (1 << bit)) for s in everyone if s & 1])

    def to_tree(value):
        return move(value, [(s, s + 1) for s in everyone if s & 1 == 0])

    def shift(value, step, lines):
        return move(value, [(s, s + 2 * step) for s in everyone if s & 1 == 0 and (s >> 1 & 3) in lines])

    place = leaf.astype(jnp.int32)[None]
    near_rows = near_list.T
    columns = jnp.arange(16, dtype=jnp.int32)
    heights = jnp.minimum(columns, levels - 1)
    path = jnp.where(
        columns < 8, heights * skeleton_index.shape[1] + (leaf >> heights), leaf - leaf % GROUP + columns - 8
    )
    cols = skeleton_index.reshape(-1, RANK).at[path].get(mode="promise_in_bounds").T

    payload, w = call(
        prepare_body,
        [((ROWS, DIM), BF16), ((RHS, RANK), F32)],
        [points, weights.T, leaf_basis],
        flops=10**9,
    )
    partner = move(payload, [(s, s ^ 1) for s in everyone])
    both = call(
        stack_body, [((2 * ROWS, DIM), BF16)], [place, payload, partner], smem=1)[0]
    right1 = shift(both, 1, (0, 1, 2))
    left1 = shift(both, -1, (1, 2, 3))
    right2 = shift(right1, 1, (1, 2))
    left2 = shift(left1, -1, (1, 2))

    matrices = transfer[0]
    extra = upper - 2
    held, leaf_pair = call(
        lambda *r: mask_body(upper, *r), [((upper * RANK + RHS, DIM), BF16), ((RANK, DIM), BF16)],
        [place, node_owner, matrices, w], smem=2,
    )
    arrived = to_tree(held)
    one, two, keep, send, lifted = call(
        lambda *r: first_body(upper, *r),
        [((RANK, DIM), BF16), ((RANK, DIM), BF16), ((extra, 128, DIM), BF16),
         ((RANK + extra * 128 + RHS, DIM), BF16), ((RHS, RANK), F32)],
        [place, held, arrived], smem=1,
    )
    two, keep, send, lifted = call(
        lambda *r: second_body(upper, *r),
        [((RANK, DIM), BF16), ((extra, 64, DIM), BF16), ((extra * 64 + RHS, DIM), BF16), ((RHS, RANK), F32)],
        [place, two, keep, lifted, cross(send, 1)], smem=1,
    )
    done, keep, w3 = call(
        lambda *r: third_body(upper, *r),
        [((64, DIM), BF16), ((extra - 1, 64, DIM), BF16), ((RHS, RANK), F32)],
        [keep, lifted, cross(send, 2)],
    )
    quarters = [done]
    for bit in range(3, levels - 2):
        arrived = cross(keep, bit)
        if keep.shape[0] > 1:
            done, keep = call(
                add_body, [((64, DIM), BF16), ((keep.shape[0] - 1, 64, DIM), BF16)], [keep, arrived],
            )
            quarters.append(done)
    halves = call(gather_body, [((extra, 64, DIM), BF16)], quarters + [keep, arrived])[0]
    halves = call(
        lambda *r: join_body(2, *r), [((extra, 128, DIM), BF16)], [place, halves, cross(halves, 2)], smem=1,
    )[0]
    pairs, lifted = call(
        lambda *r: join_body(1, *r), [((extra, RANK, DIM), BF16), ((2 * RHS, RANK), F32)],
        [place, halves, cross(halves, 1), w3], smem=1,
    )

    rows = call(skeleton_body, [((RANK, DIM), BF16)], [points, cols])[0]
    blocks = []
    for height in range(levels):
        last = height + 1 == levels
        outs = ([] if last else [((RANK, DIM), BF16)]) + ([((RANK, RANK), F32)] if height >= 3 else [])
        result = call(
            lambda *refs: node_body(height, last, *refs),
            outs,
            [place, cols, rows, cross(rows, height) if height else to_tree(rows)],
            smem=1,
        )
        if height >= 3:
            blocks.append(result[-1])
        rows = result[0]

    coeffs = []
    for height in range(3, levels - 1):
        if height > 3:
            lifted = call(
                lambda *r: climb_body(height - 3, *r), [((2 * RHS, RANK), F32)], [lifted, arrived, pairs],
            )[0]
        arrived = cross(lifted, height)
        coeffs.append(arrived)
    top = lifted[:RHS] + arrived[:RHS]
    coeffs.append(cross(top, levels - 1))
    parent = call(
        lambda *refs: descend_body(levels, *refs), [((RHS, RANK), F32)],
        [place, one, two, pairs] + blocks + coeffs, smem=1,
    )[0]
    parent_other = move(parent, [(s, s - 1) for s in everyone if s & 1])

    sums = [((2, RHS, PTS), F32), ((2, RHS, RANK), F32)]
    shared = [place, near_rows, cols]
    near, far, z, norm_z, norm_x = call(
        self_body, sums + [((2, RANK, DIM), BF16), ((2, 8, RANK), F32), ((2, 8, PTS), F32)], shared + [both],
        smem=2, flops=5 * 10**9,
    )
    near, far = call(
        lambda *r: group_body(True, *r), sums, shared + [z, norm_z, norm_x, near, far, both, right1, left1],
        smem=2, flops=10**10,
    )
    proxy = call(
        proxy_body, [((2, RHS, PTS + RANK), F32)], shared + [right1, left1, right2, left2],
        smem=2,
        scratch=[pltpu.VMEM((2, RHS, PTS), F32), pltpu.VMEM((2, RHS, RANK), F32), pltpu.VMEM((RANK, DIM), BF16)],
        flops=5 * 10**9,
    )[0]
    workers = [s for s in everyone if s & 1 == 0 and (s >> 1 & 3) in (1, 2)]
    step = lambda s: 2 if (s >> 1 & 3) == 2 else -2
    even = move(proxy[0], [(s, s + step(s)) for s in workers])
    odd = move(proxy[1], [(s, s + step(s) + 1) for s in workers])
    near, far = call(
        lambda *r: group_body(False, *r), sums, shared + [z, norm_z, norm_x, near, far, both, right2, left2],
        smem=2, flops=5 * 10**9,
    )
    handed = move(jnp.concatenate([near[1], far[1]], 1), [(s, s + 1) for s in everyone if s & 1 == 0])
    out = call(
        final_body, [((RHS, PTS), F32)],
        [place, near, far, handed, even, odd, leaf_basis, leaf_pair, parent, parent_other], smem=1, flops=10**9,
    )[0]
    return out.T


def solution(mesh):
    return jax.shard_map(
        whole,
        mesh=mesh,
        in_specs=(
            P("leaf", None),
            P("leaf", None),
            P("leaf", None),
            P("leaf", None, None, None),
            P(),
            P(),
            P(),
        ),
        out_specs=P("leaf", None),
        check_vma=False,
    )
```
